256 devices in a mesh: query: 8 (over y, z_hi), ctx: 32 (over x, z_lo, core).
Axes of the slice: x: 4, y: 4, z: 8 (z_hi: 2, z_lo: 4; z = z_hi * 4 + z_lo), core: 2. Of those that a mesh axis runs over, the one named last changes fastest.
Arguments:
- query_states: bfloat16 [256, 3072], P('query'), may hold values from -370 to 370
- key_states: bfloat16 [32768, 3072], P('ctx', 'query'), may hold values from -10.5 to 10.5
- value_states: bfloat16 [32768, 3072], P('ctx', 'query'), may hold values from -6 to 6
- level_ids: int32 [32768], P('ctx'), may hold values from 0 to 4, as said below
- level_bias: float32 [5, 24], replicated, may hold values from -1.5 to 1.5
- live_counts: int32 [32], P('ctx'), may hold values from 256 to 1024, as said below
- out_grad: bfloat16 [256, 3072], P('query'), may hold values from -6 to 6
Outputs:
- attn_out: bfloat16 [256, 3072], P(('query', 'ctx'))
- query_grad: bfloat16 [256, 3072], P(('query', 'ctx'))
- key_grad: bfloat16 [32768, 3072], P('ctx', 'query')
- value_grad: bfloat16 [32768, 3072], P('ctx', 'query')
The draws below stay inside these ranges and needn't reach their ends.
Inputs may be any that keep to these rules, and one draw needn't show every extreme that they name: Owner c's slots c * 1024 to c * 1024 + live_counts[c] - 1 are live, its other slots are empty; at least one owner has all 1024 slots live. `level_ids`: constant over each aligned run of 16 slots.
All inputs are finite; a program needn't handle non-finite values.
Results may differ from the reference program's by a relative error of at most 0.012.
Values may be sent and summed in bfloat16 or wider, within the bound.
A program may use at most 64 MiB of HBM per device.

```python
import math
import jax
import jax.numpy as jnp
from jax import lax

HEADS = 24
HEAD_DIM = 128
WIDTH = 3072
LEVELS = 5
FRAME_SLOTS = 16
QDEV = 32
CDEV = 1024
NQ = 256
NC = 32768
OWNERS = 32
N_QUERY = 8


def shared_keys(key):
    base = jnp.clip(jax.random.normal(jax.random.fold_in(key, 101), (NC, WIDTH), jnp.float32), -5.0, 5.0)
    return base


def draw_key_states(key, part):
    return shared_keys(key).astype(jnp.bfloat16)


def draw_query_states(key, part):
    queries = jnp.clip(jax.random.normal(jax.random.fold_in(key, 111), (NQ, WIDTH), jnp.float32), -5.0, 5.0)
    return queries.astype(jnp.bfloat16)


def draw_level_ids(key, part):
    frame_levels = jax.random.randint(jax.random.fold_in(key, 201), (NC // FRAME_SLOTS,), 0, LEVELS, jnp.int32)
    return jnp.repeat(frame_levels, FRAME_SLOTS)


def draw_live_counts(key, part):
    counts = jax.random.randint(jax.random.fold_in(key, 301), (OWNERS,), CDEV // 4, CDEV + 1, jnp.int32)
    full_owner = jax.random.randint(jax.random.fold_in(key, 302), (), 0, OWNERS, jnp.int32)
    owner_index = lax.iota(jnp.int32, OWNERS)
    return jnp.where(owner_index == full_owner, CDEV, counts).astype(jnp.int32)


def steps_of(key, shape, cuts, least, largest):
    def one(position, blocks):
        steps = jax.random.uniform(jax.random.fold_in(jax.random.fold_in(key, 6), position), (blocks,), jnp.float32, least / len(cuts), largest / len(cuts))
        return jnp.repeat(jnp.exp(steps), shape[position] // blocks).reshape((-1,) + (1,) * (len(shape) - position - 1))

    level = one(*cuts[0])
    for cut in cuts[1:]:
        level = level * one(*cut)
    return level


def bell_draw(own_key, shape, scale, reach, pieces=(), held_as=jnp.bfloat16):
    result = scale * jax.random.normal(own_key, shape, jnp.float32)
    if pieces:
        result = result * steps_of(own_key, shape, pieces, -0.22, 0.18)
    return jnp.clip(result, -reach, reach).astype(held_as)


def setup_inputs(seed: int = 0) -> dict:
    streams_of = jax.random.split(jax.random.key(seed), 8)
    return {
        "query_states": draw_query_states(jax.random.fold_in(streams_of[7], 71), 0),
        "key_states": draw_key_states(jax.random.fold_in(streams_of[7], 71), 0),
        "value_states": bell_draw(streams_of[2], (NC, WIDTH), 1.0, 6.0, ((0, 32), (1, 8))),
        "level_ids": draw_level_ids(jax.random.fold_in(streams_of[7], 71), 0),
        "level_bias": jnp.clip(jax.random.uniform(streams_of[4], (LEVELS, HEADS), jnp.float32, -1.5, 1.5), -1.5, 1.5),
        "live_counts": draw_live_counts(jax.random.fold_in(streams_of[7], 71), 0),
        "out_grad": bell_draw(streams_of[6], (NQ, WIDTH), 1.0, 6.0, ((0, 8),)),
    }


def reference(query_states, key_states, value_states, level_ids, level_bias, live_counts, out_grad):
    softmax_scale = 1.0 / math.sqrt(HEAD_DIM)
    level_term = level_bias[level_ids]
    slot_index = jnp.arange(NC, dtype=jnp.int32)
    live_slots = slot_index % CDEV < jnp.repeat(live_counts, CDEV)
    key_heads = key_states.astype(jnp.float32).reshape(NC, HEADS, HEAD_DIM)
    value_heads = value_states.astype(jnp.float32).reshape(NC, HEADS, HEAD_DIM)
    value_blocks = value_heads.reshape(OWNERS, CDEV, HEADS, HEAD_DIM)
    query_blocks = query_states.reshape(N_QUERY, QDEV, HEADS, HEAD_DIM)
    grad_blocks = out_grad.reshape(N_QUERY, QDEV, HEADS, HEAD_DIM)

    def query_block(carry, blocks):
        block_queries, block_grads = blocks
        queries = block_queries.astype(jnp.float32)
        grad_heads = block_grads.astype(jnp.float32)
        scores = jnp.einsum('qhd,khd->hqk', queries, key_heads) * softmax_scale + level_term.T[:, None, :]
        scores = jnp.where(live_slots[None, None, :], scores, -1e+30)
        grouped = scores.reshape(HEADS, QDEV, OWNERS, CDEV)
        block_max = lax.optimization_barrier(jnp.max(grouped, axis=3))
        raw_weights = jnp.exp(grouped - block_max[..., None])
        block_sum = lax.optimization_barrier(jnp.sum(raw_weights, axis=3))
        rounded = lax.optimization_barrier(raw_weights.astype(jnp.bfloat16)).astype(jnp.float32)
        block_out = jnp.einsum('hqck,ckhd->hqcd', rounded, value_blocks)
        row_max = lax.optimization_barrier(jnp.max(block_max, axis=2))
        factor = jnp.exp(block_max - row_max[..., None])
        total = lax.optimization_barrier(jnp.sum(factor * block_sum, axis=2))
        attention = lax.optimization_barrier(jnp.sum(factor[..., None] * block_out, axis=2)) / total[..., None]
        log_total = row_max + jnp.log(total)
        deltas = lax.optimization_barrier(jnp.sum(jnp.transpose(grad_heads, (1, 0, 2)) * attention, axis=2))
        probabilities = jnp.exp(scores - log_total[..., None])
        dprobs = jnp.einsum('qhd,khd->hqk', grad_heads, value_heads)
        dscores = lax.optimization_barrier((probabilities * (dprobs - deltas[..., None])).astype(jnp.bfloat16)).astype(jnp.float32)
        prob_rounded = lax.optimization_barrier(probabilities.astype(jnp.bfloat16)).astype(jnp.float32)
        key_part = softmax_scale * jnp.einsum('hqk,qhd->khd', dscores, queries)
        value_part = jnp.einsum('hqk,qhd->khd', prob_rounded, grad_heads)
        query_part = softmax_scale * jnp.einsum('hqk,khd->qhd', dscores, key_heads)
        key_sum, value_sum = carry
        key_sum = key_sum + lax.optimization_barrier(key_part.reshape(NC, WIDTH).astype(jnp.bfloat16)).astype(jnp.float32)
        value_sum = value_sum + lax.optimization_barrier(value_part.reshape(NC, WIDTH).astype(jnp.bfloat16)).astype(jnp.float32)
        attn_rows = jnp.transpose(attention, (1, 0, 2)).reshape(QDEV, WIDTH)
        return ((key_sum, value_sum), (attn_rows, query_part.reshape(QDEV, WIDTH)))
    start = (jnp.zeros((NC, WIDTH), jnp.float32), jnp.zeros((NC, WIDTH), jnp.float32))
    sums, stacked = lax.scan(query_block, start, (query_blocks, grad_blocks))
    attn_out = stacked[0].reshape(NQ, WIDTH).astype(jnp.bfloat16)
    query_grad = stacked[1].reshape(NQ, WIDTH).astype(jnp.bfloat16)
    return (attn_out, query_grad, sums[0].astype(jnp.bfloat16), sums[1].astype(jnp.bfloat16))
```

```python
import math

import jax
import jax.numpy as jnp
from jax import lax
from jax.experimental import pallas as pl
from jax.experimental.pallas import tpu as pltpu
from jax.sharding import PartitionSpec as P

MESH = pl.DeviceIdType.MESH
F32 = jnp.float32
BF16 = jnp.bfloat16
HD = 128
HEADS = 3
COLS = HEADS * HD
ROWS = 256
SLOTS = 1024
CHUNK = 256
SCALE = 1.0 / math.sqrt(HD)
NT = (((1,), (1,)), ((), ()))
DEAD = -1e30


def dot_nt(a, b):
    return lax.dot_general(a, b, NT, preferred_element_type=F32)


def dot(a, b):
    return jnp.dot(a, b, preferred_element_type=F32)


def kernel(
    q_hbm, k_hbm, v_hbm, lid_hbm, lb_hbm, lc_hbm, g_hbm,
    attn_ref, dq_ref, kg_hbm, vg_hbm,
    own, gat, kv, kvt, bias, perm, w32, w16, dp, pb, dsb, ot, mx,
    sx, sz, sf, rx, fb, sy, ry, kvg, lid, lb, lc,
    ld, outsem, bsend, brecv, dsend, drecv, xsend, xrecv, zsend, zrecv,
    fsend, frecv, ysend, yrecv,
):
    q = lax.axis_index("query")
    c = lax.axis_index("ctx")
    y, zh = q // 2, q % 2
    x, zl, k = c // 8, (c // 2) % 4, c % 2
    g = x * 2 + k

    loads = [
        pltpu.make_async_copy(q_hbm, own.at[0], ld.at[0]),
        pltpu.make_async_copy(g_hbm, own.at[1], ld.at[1]),
        pltpu.make_async_copy(
            q_hbm.at[:, pl.ds(pl.multiple_of(q * COLS, HD), COLS)], gat.at[0, y], ld.at[2]
        ),
        pltpu.make_async_copy(
            g_hbm.at[:, pl.ds(pl.multiple_of(q * COLS, HD), COLS)], gat.at[1, y], ld.at[3]
        ),
        pltpu.make_async_copy(k_hbm, kv.at[0], ld.at[4]),
        pltpu.make_async_copy(v_hbm, kv.at[1], ld.at[5]),
        pltpu.make_async_copy(lid_hbm, lid, ld.at[6]),
        pltpu.make_async_copy(lb_hbm, lb, ld.at[7]),
        pltpu.make_async_copy(lc_hbm, lc, ld.at[8]),
    ]
    for copy in loads:
        copy.start()

    def ctx_of(xx, zz, kk):
        return xx * 8 + zz * 2 + kk

    def xk_peer(dg):
        gp = lax.rem(g + dg, 8)
        return gp, (q, ctx_of(gp // 2, zl, gp % 2))

    edge = zl % 3 == 0
    near, far = 3 - zl, 2 - zl // 3

    barrier = pltpu.get_barrier_semaphore()

    def greet(device):
        pl.semaphore_signal(barrier, inc=1, device_id=device, device_id_type=MESH)

    for dg in range(1, 8):
        greet(xk_peer(dg)[1])
    for d in range(1, 4):
        greet((lax.rem(y + d, 4) * 2 + zh, c))
        greet((q, ctx_of(x, lax.rem(zl + d, 4), k)))

    @pl.when(edge)
    def _():
        for d in range(4):
            greet((lax.rem(y + d, 4) * 2 + 1 - zh, ctx_of(x, near, k)))
            greet((lax.rem(y + d, 4) * 2 + 1 - zh, ctx_of(x, far, k)))
        pl.semaphore_wait(barrier, 21)

    @pl.when(jnp.logical_not(edge))
    def _():
        source = jnp.where(zl < 2, 3, 0)
        for d in range(4):
            greet((lax.rem(y + d, 4) * 2 + 1 - zh, ctx_of(x, source, k)))
        pl.semaphore_wait(barrier, 17)

    loads[0].wait()
    loads[1].wait()

    def block_send(yd, half, zz, slot, sem):
        qd = yd * 2 + half
        return pltpu.make_async_remote_copy(
            src_ref=own.at[k, :, pl.ds(pl.multiple_of(qd * COLS, HD), COLS)],
            dst_ref=gat.at[k, slot],
            send_sem=bsend.at[sem],
            recv_sem=brecv.at[slot],
            device_id=(qd, ctx_of(x, zz, k)),
            device_id_type=MESH,
        )

    sends = [block_send(lax.rem(y + d, 4), zh, zl, y, d) for d in (1, 3, 2)]
    cross = []
    for d in (2, 1, 3, 0):
        cross.append(block_send(lax.rem(y + d, 4), 1 - zh, far, 4 + y, 4 + d))
        cross.append(block_send(lax.rem(y + d, 4), 1 - zh, near, 4 + y, 8 + d))
    for copy in sends:
        copy.start()

    @pl.when(edge)
    def _():
        for copy in cross:
            copy.start()

    loads[6].wait()
    loads[7].wait()
    loads[8].wait()
    live = lc[0]

    def fill(t, carry):
        level = lid[t * 16]
        alive = lax.broadcasted_iota(jnp.int32, (16, HD), 0) + t * 16 < live
        for h in range(HEADS):
            bias[h, pl.ds(pl.multiple_of(t * 16, 16), 16), :] = jnp.where(
                alive, lb[level, q * HEADS + h], DEAD
            )
        return carry

    lax.fori_loop(0, SLOTS // 16, fill, 0)

    p_id = lax.broadcasted_iota(jnp.int32, (ROWS, ROWS), 0)
    i_id = lax.broadcasted_iota(jnp.int32, (ROWS, ROWS), 1)
    p_row = ((p_id >> 6) << 3) + (((p_id >> 3) & 3) << 1) + ((p_id >> 5) & 1)
    p_half = (p_id & 1) ^ zh
    place = (p_half << 7) + (((p_id >> 1) & 3) << 5) + p_row
    perm[...] = jnp.where(i_id == place, 1.0, 0.0).astype(BF16)
    fb[...] = jnp.zeros_like(fb)
    sx[pl.ds(g, 1)] = jnp.zeros((1, 8, ROWS), F32)

    loads[4].wait()
    loads[5].wait()
    for a in range(2):
        for h in range(HEADS):
            for t in range(SLOTS // CHUNK):
                rows = slice(t * CHUNK, (t + 1) * CHUNK)
                kvt[a, h * HD : (h + 1) * HD, rows] = kv[a, rows, h * HD : (h + 1) * HD].T
    loads[2].wait()
    loads[3].wait()

    partner = (q, ctx_of(x, zl, 1 - k))

    def pass_on(slot):
        return pltpu.make_async_remote_copy(
            src_ref=gat.at[k, slot],
            dst_ref=gat.at[k, slot],
            send_sem=dsend.at[slot],
            recv_sem=drecv.at[slot],
            device_id=partner,
            device_id_type=MESH,
        )

    def from_partner(slot):
        return pltpu.make_async_remote_copy(
            src_ref=gat.at[1 - k, slot],
            dst_ref=gat.at[1 - k, slot],
            send_sem=dsend.at[slot],
            recv_sem=drecv.at[slot],
            device_id=partner,
            device_id_type=MESH,
        )

    def arrived(slot):
        return pltpu.make_async_remote_copy(
            src_ref=gat.at[k, slot],
            dst_ref=gat.at[k, slot],
            send_sem=bsend.at[0],
            recv_sem=brecv.at[slot],
            device_id=partner,
            device_id_type=MESH,
        )

    def heads_of(a, h, lo, n):
        return gat[a, lo : lo + n, :, h * HD : (h + 1) * HD].reshape(n * 32, HD)

    def forward(half):
        lanes = slice(half * HD, (half + 1) * HD)
        for h in range(HEADS):
            cols = slice(h * HD, (h + 1) * HD)
            queries = heads_of(0, h, half * 4, 4)
            peak = jnp.full((1, HD), DEAD, F32)
            for t in range(SLOTS // CHUNK):
                rows = slice(t * CHUNK, (t + 1) * CHUNK)
                score = dot_nt(kv[0, rows, cols], queries) * SCALE + bias[h, rows, :]
                w32[h, rows, lanes] = score
                peak = jnp.maximum(peak, jnp.max(score, axis=0, keepdims=True))
            total = jnp.zeros((1, HD), F32)
            for t in range(SLOTS // CHUNK):
                rows = slice(t * CHUNK, (t + 1) * CHUNK)
                weight = jnp.exp(w32[h, rows, lanes] - peak)
                w32[h, rows, lanes] = weight
                w16[h, rows, lanes] = weight.astype(BF16)
                total = total + jnp.sum(weight, axis=0, keepdims=True)
            out = dot(kvt[1, cols, :], w16[h, :, lanes])
            ot[h, :, lanes] = out
            grads = heads_of(1, h, half * 4, 4).T.astype(F32)
            product = jnp.sum(out * grads, axis=0, keepdims=True)
            mx[h : h + 1, lanes] = peak
            sx[pl.ds(g, 1), h : h + 1, lanes] = (peak + jnp.log(total)).reshape(1, 1, HD)
            sx[pl.ds(g, 1), 4 + h : 5 + h, lanes] = (product / total).reshape(1, 1, HD)

    passed = []
    for half in range(2):
        slots = [lax.rem(y + d, 4) for d in (1, 3, 2)] if half == 0 else [4, 5, 6, 7]
        for slot in slots:
            arrived(slot).wait_recv()
            copy = pass_on(slot)
            copy.start()
            passed.append(copy)
        for slot in slots:
            from_partner(slot).wait_recv()
        forward(half)

    stat_sends = []
    for dg in range(1, 8):
        gp, device = xk_peer(dg)
        copy = pltpu.make_async_remote_copy(
            src_ref=sx.at[g], dst_ref=sx.at[g], send_sem=xsend.at[gp], recv_sem=xrecv.at[g],
            device_id=device, device_id_type=MESH,
        )
        copy.start()
        stat_sends.append(copy)

    for h in range(HEADS):
        for t in range(SLOTS // CHUNK):
            rows = slice(t * CHUNK, (t + 1) * CHUNK)
            dp[h, rows, :] = dot_nt(kv[1, rows, h * HD : (h + 1) * HD], heads_of(1, h, 0, 8))

    def merge(parts):
        logs, means = parts[:, 0:4, :], parts[:, 4:8, :]
        top = jnp.max(logs, axis=0)
        share = jnp.exp(logs - top[None])
        whole = jnp.sum(share, axis=0)
        return top + jnp.log(whole), jnp.sum(share * means, axis=0) / whole

    for dg in range(1, 8):
        gp, device = xk_peer(dg)
        pltpu.make_async_remote_copy(
            src_ref=sx.at[gp], dst_ref=sx.at[gp], send_sem=xsend.at[gp], recv_sem=xrecv.at[gp],
            device_id=device, device_id_type=MESH,
        ).wait_recv()
    logs, means = merge(sx[...])
    sz[pl.ds(zl, 1), 0:4, :] = logs[None]
    sz[pl.ds(zl, 1), 4:8, :] = means[None]
    for d in range(1, 4):
        zp = lax.rem(zl + d, 4)
        copy = pltpu.make_async_remote_copy(
            src_ref=sz.at[zl], dst_ref=sz.at[zl], send_sem=zsend.at[zp], recv_sem=zrecv.at[zl],
            device_id=(q, ctx_of(x, zp, k)), device_id_type=MESH,
        )
        copy.start()
        stat_sends.append(copy)
    for d in range(1, 4):
        zp = lax.rem(zl + d, 4)
        pltpu.make_async_remote_copy(
            src_ref=sz.at[zp], dst_ref=sz.at[zp], send_sem=zsend.at[zp], recv_sem=zrecv.at[zp],
            device_id=(q, ctx_of(x, zp, k)), device_id_type=MESH,
        ).wait_recv()
    log_total, deltas = merge(sz[...])

    factor = [jnp.exp(mx[h : h + 1, :] - log_total[h : h + 1, :]) for h in range(HEADS)]

    def to_owner_rows(a, h, turned):
        rows = dot_nt(perm[...], turned.astype(BF16)).astype(BF16)
        sf[a, :, :, h * HD : (h + 1) * HD] = rows.reshape(8, 32, HD)

    def send_rows(a):
        for dg in range(1, 8):
            gp, device = xk_peer(dg)
            copy = pltpu.make_async_remote_copy(
                src_ref=sf.at[a, gp], dst_ref=rx.at[a, g],
                send_sem=fsend.at[a, gp], recv_sem=frecv.at[a, g],
                device_id=device, device_id_type=MESH,
            )
            copy.start()
            stat_sends.append(copy)

    for h in range(HEADS):
        to_owner_rows(0, h, ot[h] * factor[h])
    send_rows(0)

    for h in range(HEADS):
        for t in range(SLOTS // HD):
            rows = slice(t * HD, (t + 1) * HD)
            prob = w32[h, rows, :] * factor[h]
            pb[h, rows, :] = prob.astype(BF16)
            dsb[h, rows, :] = (prob * (dp[h, rows, :] - deltas[h : h + 1, :])).astype(BF16)
        to_owner_rows(1, h, dot(kvt[0, h * HD : (h + 1) * HD, :], dsb[h]) * SCALE)
    send_rows(1)

    for h in range(HEADS):
        cols = slice(h * HD, (h + 1) * HD)
        for t in range(SLOTS // CHUNK):
            rows = slice(t * CHUNK, (t + 1) * CHUNK)
            kvg[0, rows, cols] = (dot(dsb[h, rows, :], heads_of(0, h, 0, 8)) * SCALE).astype(BF16)
            kvg[1, rows, cols] = dot(pb[h, rows, :], heads_of(1, h, 0, 8)).astype(BF16)
    outs = [
        pltpu.make_async_copy(kvg.at[0], kg_hbm, outsem.at[0]),
        pltpu.make_async_copy(kvg.at[1], vg_hbm, outsem.at[1]),
    ]
    for copy in outs:
        copy.start()

    for a in range(2):
        rx[a, pl.ds(g, 1)] = sf[a, pl.ds(g, 1)]
        for dg in range(1, 8):
            gp, device = xk_peer(dg)
            pltpu.make_async_remote_copy(
                src_ref=sf.at[a, gp], dst_ref=rx.at[a, gp],
                send_sem=fsend.at[a, gp], recv_sem=frecv.at[a, gp],
                device_id=device, device_id_type=MESH,
            ).wait_recv()
        summed = jnp.sum(rx[a].astype(F32), axis=0)
        for h in range(HEADS):
            fb[pl.ds(a * HEADS + h, 32, stride=8), :] = summed[:, h * HD : (h + 1) * HD]
    sy[...] = fb[...].astype(BF16).reshape(32, 8, HD)

    me = zl * 8 + q

    def row_copy(dz, dq, out):
        zp, qp = lax.rem(zl + dz, 4), lax.rem(q + dq, 8)
        d = zp * 8 + qp
        return pltpu.make_async_remote_copy(
            src_ref=sy.at[d], dst_ref=ry.at[me] if out else ry.at[d],
            send_sem=ysend.at[d], recv_sem=yrecv.at[me] if out else yrecv.at[d],
            device_id=(qp, ctx_of(x, zp, k)), device_id_type=MESH,
        )

    steps = [(dz, dq) for dz in range(4) for dq in range(8) if dz or dq]
    for dz, dq in steps:
        copy = row_copy(dz, dq, True)
        copy.start()
        stat_sends.append(copy)
    ry[pl.ds(me, 1)] = sy[pl.ds(me, 1)]
    for dz, dq in steps:
        row_copy(dz, dq, False).wait_recv()
    final = jnp.sum(ry[...].astype(F32).reshape(4, 8, 8, HD), axis=0)
    for qd in range(8):
        for h in range(HEADS):
            cols = slice((qd * HEADS + h) * HD, (qd * HEADS + h + 1) * HD)
            attn_ref[:, cols] = final[qd, h : h + 1, :].astype(BF16)
            dq_ref[:, cols] = final[qd, HEADS + h : HEADS + h + 1, :].astype(BF16)

    for copy in sends + passed + stat_sends:
        copy.wait_send()

    @pl.when(edge)
    def _():
        for copy in cross:
            copy.wait_send()

    for copy in outs:
        copy.wait()


def local(query_states, key_states, value_states, level_ids, level_bias, live_counts, out_grad):
    hbm = pl.BlockSpec(memory_space=pltpu.HBM)
    vmem = pl.BlockSpec(memory_space=pltpu.VMEM)
    dma = pltpu.SemaphoreType.DMA
    return pl.pallas_call(
        kernel,
        name="framepack",
        out_shape=(
            jax.ShapeDtypeStruct((1, 3072), BF16),
            jax.ShapeDtypeStruct((1, 3072), BF16),
            jax.ShapeDtypeStruct(key_states.shape, BF16),
            jax.ShapeDtypeStruct(value_states.shape, BF16),
        ),
        in_specs=[hbm] * 7,
        out_specs=(vmem, vmem, hbm, hbm),
        scratch_shapes=[
            pltpu.VMEM((2, 32, 3072), BF16),
            pltpu.VMEM((2, 8, 32, COLS), BF16),
            pltpu.VMEM((2, SLOTS, COLS), BF16),
            pltpu.VMEM((2, COLS, SLOTS), BF16),
            pltpu.VMEM((HEADS, SLOTS, HD), F32),
            pltpu.VMEM((ROWS, ROWS), BF16),
            pltpu.VMEM((HEADS, SLOTS, ROWS), F32),
            pltpu.VMEM((HEADS, SLOTS, ROWS), BF16),
            pltpu.VMEM((HEADS, SLOTS, ROWS), F32),
            pltpu.VMEM((HEADS, SLOTS, ROWS), BF16),
            pltpu.VMEM((HEADS, SLOTS, ROWS), BF16),
            pltpu.VMEM((HEADS, HD, ROWS), F32),
            pltpu.VMEM((8, ROWS), F32),
            pltpu.VMEM((8, 8, ROWS), F32),
            pltpu.VMEM((4, 8, ROWS), F32),
            pltpu.VMEM((2, 8, 32, COLS), BF16),
            pltpu.VMEM((2, 8, 32, COLS), BF16),
            pltpu.VMEM((ROWS, HD), F32),
            pltpu.VMEM((32, 8, HD), BF16),
            pltpu.VMEM((32, 8, HD), BF16),
            pltpu.VMEM((2, SLOTS, COLS), BF16),
            pltpu.SMEM((SLOTS,), jnp.int32),
            pltpu.SMEM((5, 24), F32),
            pltpu.SMEM((1,), jnp.int32),
            dma((9,)), dma((2,)),
            dma((12,)), dma((8,)),
            dma((8,)), dma((8,)),
            dma((8,)), dma((8,)),
            dma((4,)), dma((4,)),
            dma((2, 8)), dma((2, 8)),
            dma((32,)), dma((32,)),
        ],
        compiler_params=pltpu.CompilerParams(
            collective_id=0, has_side_effects=True, vmem_limit_bytes=56 * 1024 * 1024
        ),
    )(query_states, key_states, value_states, level_ids, level_bias, live_counts, out_grad)


def solution(mesh):
    placed = (
        P("query", None),
        P("ctx", "query"),
        P("ctx", "query"),
        P("ctx"),
        P(),
        P("ctx"),
        P("query", None),
    )
    return jax.shard_map(
        local,
        mesh=mesh,
        in_specs=placed,
        out_specs=(
            P(("query", "ctx"), None),
            P(("query", "ctx"), None),
            P("ctx", "query"),
            P("ctx", "query"),
        ),
        check_vma=False,
    )
```

```python
import math

import jax
import jax.numpy as jnp
from jax import lax
from jax.experimental import pallas as pl
from jax.experimental.pallas import tpu as pltpu
from jax.sharding import PartitionSpec as P

MESH = pl.DeviceIdType.MESH
F32 = jnp.float32
BF16 = jnp.bfloat16
HD = 128
HEADS = 3
COLS = HEADS * HD
ROWS = 256
SLOTS = 1024
CHUNK = 256
SCALE = 1.0 / math.sqrt(HD)
NT = (((1,), (1,)), ((), ()))
DEAD = -1e30


def dot_nt(a, b):
    return lax.dot_general(a, b, NT, preferred_element_type=F32)


def dot(a, b):
    return jnp.dot(a, b, preferred_element_type=F32)


def kernel(
    q_hbm, k_hbm, v_hbm, lid_hbm, lb_hbm, lc_hbm, g_hbm,
    attn_ref, dq_ref, kg_ref, vg_ref,
    own, gat, kv, kvt, bias, perm, w32, w16, dp, pb, dsb, mx,
    sx, sz, sf, rx, fb, sy, ry, lid, lb, lc,
    ld, bsend, brecv, dsend, drecv, xsend, xrecv, zsend, zrecv,
    fsend, frecv, ysend, yrecv,
):
    q = lax.axis_index("query")
    c = lax.axis_index("ctx")
    y, zh = q // 2, q % 2
    x, zl, k = c // 8, (c // 2) % 4, c % 2
    g = x * 2 + k

    loads = [
        pltpu.make_async_copy(q_hbm, own.at[0], ld.at[0]),
        pltpu.make_async_copy(g_hbm, own.at[1], ld.at[1]),
        pltpu.make_async_copy(
            q_hbm.at[:, pl.ds(pl.multiple_of(q * COLS, HD), COLS)], gat.at[0, y], ld.at[2]
        ),
        pltpu.make_async_copy(
            g_hbm.at[:, pl.ds(pl.multiple_of(q * COLS, HD), COLS)], gat.at[1, y], ld.at[3]
        ),
        pltpu.make_async_copy(k_hbm, kv.at[0], ld.at[4]),
        pltpu.make_async_copy(v_hbm, kv.at[1], ld.at[5]),
        pltpu.make_async_copy(lid_hbm, lid, ld.at[6]),
        pltpu.make_async_copy(lb_hbm, lb, ld.at[7]),
        pltpu.make_async_copy(lc_hbm, lc, ld.at[8]),
    ]
    for copy in loads:
        copy.start()

    def ctx_of(xx, zz, kk):
        return xx * 8 + zz * 2 + kk

    def xk_peer(dg):
        gp = lax.rem(g + dg, 8)
        return gp, (q, ctx_of(gp // 2, zl, gp % 2))

    edge = zl % 3 == 0
    near, far = 3 - zl, 2 - zl // 3

    barrier = pltpu.get_barrier_semaphore()

    def greet(device):
        pl.semaphore_signal(barrier, inc=1, device_id=device, device_id_type=MESH)

    for dg in range(1, 8):
        greet(xk_peer(dg)[1])
    for d in range(1, 4):
        greet((lax.rem(y + d, 4) * 2 + zh, c))
        greet((q, ctx_of(x, lax.rem(zl + d, 4), k)))

    @pl.when(edge)
    def _():
        for d in range(4):
            greet((lax.rem(y + d, 4) * 2 + 1 - zh, ctx_of(x, near, k)))
            greet((lax.rem(y + d, 4) * 2 + 1 - zh, ctx_of(x, far, k)))
        pl.semaphore_wait(barrier, 21)

    @pl.when(jnp.logical_not(edge))
    def _():
        source = jnp.where(zl < 2, 3, 0)
        for d in range(4):
            greet((lax.rem(y + d, 4) * 2 + 1 - zh, ctx_of(x, source, k)))
        pl.semaphore_wait(barrier, 17)

    loads[0].wait()
    loads[1].wait()

    def block_send(yd, half, zz, slot, sem):
        qd = yd * 2 + half
        return pltpu.make_async_remote_copy(
            src_ref=own.at[k, :, pl.ds(pl.multiple_of(qd * COLS, HD), COLS)],
            dst_ref=gat.at[k, slot],
            send_sem=bsend.at[sem],
            recv_sem=brecv.at[slot],
            device_id=(qd, ctx_of(x, zz, k)),
            device_id_type=MESH,
        )

    sends = [block_send(lax.rem(y + d, 4), zh, zl, y, d) for d in (1, 3, 2)]
    cross = []
    for d in (2, 1, 3, 0):
        cross.append(block_send(lax.rem(y + d, 4), 1 - zh, far, 4 + y, 4 + d))
        cross.append(block_send(lax.rem(y + d, 4), 1 - zh, near, 4 + y, 8 + d))
    for copy in sends:
        copy.start()

    @pl.when(edge)
    def _():
        for copy in cross:
            copy.start()

    loads[6].wait()
    loads[7].wait()
    loads[8].wait()
    live = lc[0]

    def fill(t, carry):
        level = lid[t * 16]
        alive = lax.broadcasted_iota(jnp.int32, (16, HD), 0) + t * 16 < live
        for h in range(HEADS):
            bias[h, pl.ds(pl.multiple_of(t * 16, 16), 16), :] = jnp.where(
                alive, lb[level, q * HEADS + h], DEAD
            )
        return carry

    lax.fori_loop(0, SLOTS // 16, fill, 0)

    p_id = lax.broadcasted_iota(jnp.int32, (HD, HD), 0)
    i_id = lax.broadcasted_iota(jnp.int32, (HD, HD), 1)
    p_row = ((p_id >> 5) << 3) + (((p_id >> 2) & 3) << 1) + ((p_id >> 4) & 1)
    perm[...] = jnp.where(i_id == ((p_id & 3) << 5) + p_row, 1.0, 0.0).astype(F32)
    own_rows = lax.broadcasted_iota(jnp.int32, (16, HD), 0)
    own_lane = ((own_rows & 3) << 5) + x * 8 + ((own_rows >> 2) << 1) + k
    pick = jnp.where(lax.broadcasted_iota(jnp.int32, (16, HD), 1) == own_lane, 1.0, 0.0)
    fb[...] = jnp.zeros_like(fb)
    for half in range(2):
        sx[half, pl.ds(g, 1)] = jnp.zeros((1, 8, HD), F32)

    loads[4].wait()
    loads[5].wait()
    for a in range(2):
        for h in range(HEADS):
            for t in range(SLOTS // CHUNK):
                rows = slice(t * CHUNK, (t + 1) * CHUNK)
                kvt[h, (1 - a) * HD : (2 - a) * HD, rows] = kv[a, rows, h * HD : (h + 1) * HD].T
    loads[2].wait()
    loads[3].wait()

    partner = (q, ctx_of(x, zl, 1 - k))

    def pass_on(slot):
        return pltpu.make_async_remote_copy(
            src_ref=gat.at[k, slot],
            dst_ref=gat.at[k, slot],
            send_sem=dsend.at[slot],
            recv_sem=drecv.at[slot],
            device_id=partner,
            device_id_type=MESH,
        )

    def from_partner(slot):
        return pltpu.make_async_remote_copy(
            src_ref=gat.at[1 - k, slot],
            dst_ref=gat.at[1 - k, slot],
            send_sem=dsend.at[slot],
            recv_sem=drecv.at[slot],
            device_id=partner,
            device_id_type=MESH,
        )

    def arrived(slot):
        return pltpu.make_async_remote_copy(
            src_ref=gat.at[k, slot],
            dst_ref=gat.at[k, slot],
            send_sem=bsend.at[0],
            recv_sem=brecv.at[slot],
            device_id=partner,
            device_id_type=MESH,
        )

    def heads_of(a, h, lo, n):
        return gat[a, lo : lo + n, :, h * HD : (h + 1) * HD].reshape(n * 32, HD)

    kept = {}

    def forward(half, h):
        lanes = slice(half * HD, (half + 1) * HD)
        cols = slice(h * HD, (h + 1) * HD)
        queries = heads_of(0, h, half * 4, 4)
        peak = jnp.full((1, HD), DEAD, F32)
        for t in range(SLOTS // CHUNK):
            rows = slice(t * CHUNK, (t + 1) * CHUNK)
            score = dot_nt(kv[0, rows, cols], queries) * SCALE + bias[h, rows, :]
            w32[h, rows, lanes] = score
            peak = jnp.maximum(peak, jnp.max(score, axis=0, keepdims=True))
        total = jnp.zeros((1, HD), F32)
        for t in range(SLOTS // CHUNK):
            rows = slice(t * CHUNK, (t + 1) * CHUNK)
            weight = jnp.exp(w32[h, rows, lanes] - peak)
            w32[h, rows, lanes] = weight
            w16[h, rows, lanes] = weight.astype(BF16)
            total = total + jnp.sum(weight, axis=0, keepdims=True)
        inverse = 1.0 / total
        mixed = dot(kvt[h], w16[h, :, lanes]) * inverse
        grads = heads_of(1, h, half * 4, 4).T.astype(F32)
        mean = jnp.sum(mixed[0:HD] * grads, axis=0, keepdims=True)
        mx[h : h + 1, lanes] = peak
        sx[half, pl.ds(g, 1), h : h + 1, :] = (peak + jnp.log(total)).reshape(1, 1, HD)
        sx[half, pl.ds(g, 1), 4 + h : 5 + h, :] = mean.reshape(1, 1, HD)
        kept[half, h] = (mixed.astype(BF16), mean, inverse)

    def stats_copy(half, gp, device, out):
        slot = g if out else gp
        return pltpu.make_async_remote_copy(
            src_ref=sx.at[half, slot], dst_ref=sx.at[half, slot],
            send_sem=xsend.at[half, gp], recv_sem=xrecv.at[half, slot],
            device_id=device, device_id_type=MESH,
        )

    stat_sends = []

    def send_stats(half):
        for dg in range(1, 8):
            gp, device = xk_peer(dg)
            copy = stats_copy(half, gp, device, True)
            copy.start()
            stat_sends.append(copy)

    def shares_copy(half, h, gp, device, out):
        return pltpu.make_async_remote_copy(
            src_ref=sf.at[half, h, gp], dst_ref=rx.at[half, h, g if out else gp],
            send_sem=fsend.at[half, h, gp], recv_sem=frecv.at[half, h, g if out else gp],
            device_id=device, device_id_type=MESH,
        )

    def shares(half, h):
        lanes = slice(half * HD, (half + 1) * HD)
        cols = slice(h * HD, (h + 1) * HD)
        mixed, mean, inverse = kept[half, h]
        grads = heads_of(1, h, half * 4, 4)
        for t in range(SLOTS // CHUNK):
            rows = slice(t * CHUNK, (t + 1) * CHUNK)
            dprob = dot_nt(kv[1, rows, cols], grads)
            dp[h, rows, lanes] = dprob
            dsb[h, rows, lanes] = (w32[h, rows, lanes] * (dprob - mean)).astype(BF16)
        slope = (dot(kvt[h, HD : 2 * HD, :], dsb[h, :, lanes]) * inverse).astype(BF16)
        turned = jnp.concatenate([mixed, slope], axis=0)
        rows = dot_nt(perm[...].astype(BF16), turned).astype(BF16)
        sf[half, h] = rows.reshape(8, 16, 3 * HD)
        for dg in range(1, 8):
            gp, device = xk_peer(dg)
            copy = shares_copy(half, h, gp, device, True)
            copy.start()
            stat_sends.append(copy)

    passed = []
    for half in range(2):
        slots = [lax.rem(y + d, 4) for d in (1, 3, 2)] if half == 0 else [4, 5, 6, 7]
        for slot in slots:
            arrived(slot).wait_recv()
            copy = pass_on(slot)
            copy.start()
            passed.append(copy)
        for slot in slots:
            from_partner(slot).wait_recv()
        for h in range(HEADS):
            forward(half, h)
        send_stats(half)
        for h in range(HEADS):
            shares(half, h)

    def merge(parts):
        logs, means = parts[:, 0:4, :], parts[:, 4:8, :]
        top = jnp.max(logs, axis=0)
        share = jnp.exp(logs - top[None])
        whole = jnp.sum(share, axis=0)
        return top + jnp.log(whole), jnp.sum(share * means, axis=0) / whole

    for half in range(2):
        for dg in range(1, 8):
            gp, device = xk_peer(dg)
            stats_copy(half, gp, device, False).wait_recv()
        logs, means = merge(sx[half])
        sz[half, pl.ds(zl, 1), 0:4, :] = logs[None]
        sz[half, pl.ds(zl, 1), 4:8, :] = means[None]

    def merged_copy(half, zp, out):
        slot = zl if out else zp
        return pltpu.make_async_remote_copy(
            src_ref=sz.at[half, slot], dst_ref=sz.at[half, slot],
            send_sem=zsend.at[half, zp], recv_sem=zrecv.at[half, slot],
            device_id=(q, ctx_of(x, zp, k)), device_id_type=MESH,
        )

    for half in range(2):
        for d in range(1, 4):
            copy = merged_copy(half, lax.rem(zl + d, 4), True)
            copy.start()
            stat_sends.append(copy)
    final_stats = []
    columns = []
    for half in range(2):
        for d in range(1, 4):
            merged_copy(half, lax.rem(zl + d, 4), False).wait_recv()
        log_total, delta = merge(sz[half])
        final_stats.append((log_total, delta))
        gain = jnp.exp(sx[half, :, 0:4, :] - log_total[None])
        tilt = gain * (sx[half, :, 4:8, :] - delta[None])
        both = jnp.concatenate([gain, tilt], axis=1).reshape(64, HD)
        columns.append(
            lax.dot_general(
                pick, both, NT, preferred_element_type=F32, precision=lax.Precision.HIGHEST
            )
        )

    for half in range(2):
        for h in range(HEADS):
            rx[half, h, pl.ds(g, 1)] = sf[half, h, pl.ds(g, 1)]
            for dg in range(1, 8):
                gp, device = xk_peer(dg)
                shares_copy(half, h, gp, device, False).wait_recv()
            attn_rows = jnp.zeros((16, HD), F32)
            grad_rows = jnp.zeros((16, HD), F32)
            for s in range(8):
                gain = columns[half][:, s * 8 + h : s * 8 + h + 1]
                tilt = columns[half][:, s * 8 + 4 + h : s * 8 + 5 + h]
                part = rx[half, h, s].astype(F32)
                attn_rows = attn_rows + gain * part[:, 0:HD]
                grad_rows = grad_rows + (tilt * part[:, HD : 2 * HD] + gain * part[:, 2 * HD :])
            fb[pl.ds(half * HD + h, 16, stride=8), :] = attn_rows
            fb[pl.ds(half * HD + HEADS + h, 16, stride=8), :] = grad_rows * SCALE
    sy[...] = fb[...].astype(BF16).reshape(32, 8, HD)

    me = zl * 8 + q

    def row_copy(rel, dz, dy, out):
        zp, yp, hp = lax.rem(zl + dz, 4), lax.rem(y + dy, 4), lax.rem(zh + rel, 2)
        e = rel * 16 + zp * 4 + yp
        qp = yp * 2 + hp
        other = zp * 8 + qp
        return pltpu.make_async_remote_copy(
            src_ref=sy.at[e], dst_ref=ry.at[me] if out else ry.at[other],
            send_sem=ysend.at[e], recv_sem=yrecv.at[me] if out else yrecv.at[other],
            device_id=(qp, ctx_of(x, zp, k)), device_id_type=MESH,
        )

    steps = [
        (rel, dz, dy)
        for rel in (1, 0) for dz in (2, 1, 3, 0) for dy in (2, 1, 3, 0)
        if rel or dz or dy
    ]
    for step in steps:
        copy = row_copy(*step, True)
        copy.start()
        stat_sends.append(copy)
    ry[pl.ds(me, 1)] = sy[pl.ds(zl * 4 + y, 1)]

    for h in range(HEADS):
        cols = slice(h * HD, (h + 1) * HD)
        factor = jnp.concatenate(
            [jnp.exp(mx[h : h + 1, half * HD : (half + 1) * HD] - final_stats[half][0][h : h + 1])
             for half in range(2)], axis=1)
        delta = jnp.concatenate([final_stats[half][1][h : h + 1] for half in range(2)], axis=1)
        for t in range(SLOTS // HD):
            rows = slice(t * HD, (t + 1) * HD)
            prob = w32[h, rows, :] * factor
            pb[h, rows, :] = prob.astype(BF16)
            dsb[h, rows, :] = (prob * (dp[h, rows, :] - delta)).astype(BF16)
        for t in range(SLOTS // CHUNK):
            rows = slice(t * CHUNK, (t + 1) * CHUNK)
            kg_ref[rows, cols] = (dot(dsb[h, rows, :], heads_of(0, h, 0, 8)) * SCALE).astype(BF16)
            vg_ref[rows, cols] = dot(pb[h, rows, :], heads_of(1, h, 0, 8)).astype(BF16)

    for step in steps:
        row_copy(*step, False).wait_recv()
    final = jnp.sum(ry[...].astype(F32).reshape(4, 8, 8, HD), axis=0)
    for qd in range(8):
        for h in range(HEADS):
            cols = slice((qd * HEADS + h) * HD, (qd * HEADS + h + 1) * HD)
            attn_ref[:, cols] = final[qd, h : h + 1, :].astype(BF16)
            dq_ref[:, cols] = final[qd, HEADS + h : HEADS + h + 1, :].astype(BF16)

    for copy in sends + passed + stat_sends:
        copy.wait_send()

    @pl.when(edge)
    def _():
        for copy in cross:
            copy.wait_send()


def write_out(attn_in, dq_in, kg_in, vg_in, attn_out, dq_out, kg_out, vg_out, sems):
    pairs = ((kg_in, kg_out), (vg_in, vg_out), (attn_in, attn_out), (dq_in, dq_out))
    copies = [pltpu.make_async_copy(a, b, sems.at[n]) for n, (a, b) in enumerate(pairs)]
    for copy in copies:
        copy.start()
    for copy in copies:
        copy.wait()


def local(query_states, key_states, value_states, level_ids, level_bias, live_counts, out_grad):
    hbm = pl.BlockSpec(memory_space=pltpu.HBM)
    vmem = pl.BlockSpec(memory_space=pltpu.VMEM)
    dma = pltpu.SemaphoreType.DMA
    arrays = (
        query_states, key_states, value_states, level_ids, level_bias, live_counts, out_grad
    )
    shapes = ((1, 3072), (1, 3072), key_states.shape, value_states.shape)
    results = pl.pallas_call(
        kernel,
        name="framepack",
        out_shape=tuple(pltpu.VMEM(shape, BF16) for shape in shapes),
        in_specs=[hbm] * 7,
        out_specs=(vmem,) * 4,
        scratch_shapes=[
            pltpu.VMEM((2, 32, 3072), BF16),
            pltpu.VMEM((2, 8, 32, COLS), BF16),
            pltpu.VMEM((2, SLOTS, COLS), BF16),
            pltpu.VMEM((HEADS, 2 * HD, SLOTS), BF16),
            pltpu.VMEM((HEADS, SLOTS, HD), F32),
            pltpu.VMEM((HD, HD), F32),
            pltpu.VMEM((HEADS, SLOTS, ROWS), F32),
            pltpu.VMEM((HEADS, SLOTS, ROWS), BF16),
            pltpu.VMEM((HEADS, SLOTS, ROWS), F32),
            pltpu.VMEM((HEADS, SLOTS, ROWS), BF16),
            pltpu.VMEM((HEADS, SLOTS, ROWS), BF16),
            pltpu.VMEM((8, ROWS), F32),
            pltpu.VMEM((2, 8, 8, HD), F32),
            pltpu.VMEM((2, 4, 8, HD), F32),
            pltpu.VMEM((2, HEADS, 8, 16, COLS), BF16),
            pltpu.VMEM((2, HEADS, 8, 16, COLS), BF16),
            pltpu.VMEM((ROWS, HD), F32),
            pltpu.VMEM((32, 8, HD), BF16),
            pltpu.VMEM((32, 8, HD), BF16),
            pltpu.SMEM((SLOTS,), jnp.int32),
            pltpu.SMEM((5, 24), F32),
            pltpu.SMEM((1,), jnp.int32),
            dma((9,)),
            dma((12,)), dma((8,)),
            dma((8,)), dma((8,)),
            dma((2, 8)), dma((2, 8)),
            dma((2, 4)), dma((2, 4)),
            dma((2, HEADS, 8)), dma((2, HEADS, 8)),
            dma((32,)), dma((32,)),
        ],
        compiler_params=pltpu.CompilerParams(
            collective_id=0, has_side_effects=True, vmem_limit_bytes=32 * 1024 * 1024
        ),
    )(*(a if a is live_counts else pltpu.with_memory_space_constraint(a, pltpu.HBM) for a in arrays))
    return pl.pallas_call(
        write_out,
        name="write_out",
        out_shape=tuple(jax.ShapeDtypeStruct(shape, BF16) for shape in shapes),
        in_specs=[vmem] * 4,
        out_specs=(hbm,) * 4,
        scratch_shapes=[dma((4,))],
    )(*(pltpu.with_memory_space_constraint(a, pltpu.VMEM) for a in results))


def solution(mesh):
    placed = (
        P("query", None),
        P("ctx", "query"),
        P("ctx", "query"),
        P("ctx"),
        P(),
        P("ctx"),
        P("query", None),
    )
    return jax.shard_map(
        local,
        mesh=mesh,
        in_specs=placed,
        out_specs=(
            P(("query", "ctx"), None),
            P(("query", "ctx"), None),
            P("ctx", "query"),
            P("ctx", "query"),
        ),
        check_vma=False,
    )
```

```python
import math

import jax
import jax.numpy as jnp
from jax import lax
from jax.experimental import pallas as pl
from jax.experimental.pallas import tpu as pltpu
from jax.sharding import PartitionSpec as P

MESH = pl.DeviceIdType.MESH
F32 = jnp.float32
BF16 = jnp.bfloat16
HD = 128
HEADS = 3
COLS = HEADS * HD
ROWS = 128
SLOTS = 1024
BOTH = 2 * SLOTS
RUNS = SLOTS // 16
CHUNK = 256
SCALE = 1.0 / math.sqrt(HD)
NT = (((1,), (1,)), ((), ()))
DEAD = -1e30


def dot_nt(a, b):
    return lax.dot_general(a, b, NT, preferred_element_type=F32)


def dot(a, b):
    return jnp.dot(a, b, preferred_element_type=F32)


def kernel(
    q_hbm, k_hbm, v_hbm, lid_hbm, lb_hbm, lc_hbm, g_hbm,
    attn_ref, dq_ref, kg_ref, vg_ref,
    own, gat, kv, kvt, table, bias, perm, w32, w16, dp, pb, dsb, mx,
    sx, sz, sf, rx, fb, sy, ry, kvo, xs, xr, lid, lb, lc,
    ld, dsend, drecv, bsend, brecv, xsend, xrecv, zsend, zrecv,
    fsend, frecv, ysend, yrecv, gsend, grecv,
):
    q = lax.axis_index("query")
    c = lax.axis_index("ctx")
    y, zh = q // 2, q % 2
    x, zl, k = c // 8, (c // 2) % 4, c % 2
    first, second = k == 0, k == 1

    def ctx_of(xx, zz, kk):
        return xx * 8 + zz * 2 + kk

    def load(src, dst, n):
        copy = pltpu.make_async_copy(src, dst, ld.at[n])
        copy.start()
        return copy

    loads = [
        load(q_hbm, own.at[0], 0),
        load(g_hbm, own.at[1], 1),
        load(lid_hbm, lid, 2),
        load(lb_hbm, lb, 3),
        load(lc_hbm, lc, 4),
        load(k_hbm, kv.at[0, 0:SLOTS], 5),
        load(v_hbm, kv.at[1, 0:SLOTS], 6),
    ]

    edge = zl % 3 == 0
    near, far = 3 - zl, 2 - zl // 3
    source = jnp.where(zl < 2, 3, 0)
    partner = (q, ctx_of(x, zl, 1 - k))
    ys = [lax.rem(y + d, 4) for d in range(4)]
    xs_of = [lax.rem(x + d, 4) for d in range(4)]
    zs = [lax.rem(zl + d, 4) for d in range(4)]
    barrier = pltpu.get_barrier_semaphore()

    def greet(device):
        pl.semaphore_signal(barrier, inc=1, device_id=device, device_id_type=MESH)

    for d in range(1, 4):
        greet((q, ctx_of(xs_of[d], zl, k)))
        greet((q, ctx_of(x, zs[d], k)))
    greet(partner)

    @pl.when(first)
    def _():
        for d in range(4):
            greet((ys[d] * 2 + 1 - zh, ctx_of(x, source, 1)))
        for d in range(1, 4):
            greet((ys[d] * 2 + zh, c))
        pl.semaphore_wait(barrier, 10)

    @pl.when(jnp.logical_and(second, edge))
    def _():
        for d in range(4):
            greet((ys[d] * 2 + 1 - zh, ctx_of(x, far, 1)))
            greet((ys[d] * 2 + 1 - zh, ctx_of(x, near, 1)))
        pl.semaphore_wait(barrier, 23)

    @pl.when(jnp.logical_and(second, jnp.logical_not(edge)))
    def _():
        for d in range(4):
            greet((ys[d] * 2 + 1 - zh, ctx_of(x, source, 1)))
        pl.semaphore_wait(barrier, 11)

    loads[0].wait()
    loads[1].wait()

    def remote(src, dst, send, recv, device):
        return pltpu.make_async_remote_copy(
            src_ref=src, dst_ref=dst, send_sem=send, recv_sem=recv,
            device_id=device, device_id_type=MESH,
        )

    def block_send(h, yd, half, zz):
        qd = yd * 2 + half
        cols = pl.ds(pl.multiple_of(qd * COLS + h * HD, HD), HD)
        remote(
            own.at[:, :, cols], gat.at[h, :, y], bsend.at[0], brecv.at[h],
            (qd, ctx_of(x, zz, k)),
        ).start()

    @pl.when(first)
    def _():
        for h in range(HEADS):
            for d in (2, 1, 3):
                block_send(h, ys[d], zh, zl)
            cols = pl.ds(pl.multiple_of(q * COLS + h * HD, HD), HD)
            gat[h, :, pl.ds(y, 1)] = own[:, :, cols].reshape(2, 1, 32, HD)

    @pl.when(jnp.logical_and(second, edge))
    def _():
        for h in range(HEADS):
            for d in (2, 1, 3, 0):
                block_send(h, ys[d], 1 - zh, far)
                block_send(h, ys[d], 1 - zh, near)

    loads[2].wait()
    loads[3].wait()
    loads[4].wait()

    def fill(t, carry):
        level = lid[t * 16]
        for h in range(HEADS):
            table[0, pl.ds(h * RUNS + t, 1), :] = jnp.full((1, HD), lb[level, q * HEADS + h], F32)
        return carry

    lax.fori_loop(0, RUNS, fill, 0)
    table[0, HEADS * RUNS :, :] = jnp.full((8, HD), lc[0].astype(F32), F32)
    loads[5].wait()
    loads[6].wait()
    swaps = [
        remote(table.at[0], table.at[1], dsend.at[0], drecv.at[0], partner),
        remote(kv.at[0, 0:SLOTS], kv.at[0, SLOTS:BOTH], dsend.at[1], drecv.at[1], partner),
        remote(kv.at[1, 0:SLOTS], kv.at[1, SLOTS:BOTH], dsend.at[2], drecv.at[2], partner),
    ]
    for copy in swaps:
        copy.start()

    p_id = lax.broadcasted_iota(jnp.int32, (HD, HD), 0)
    i_id = lax.broadcasted_iota(jnp.int32, (HD, HD), 1)
    perm[...] = jnp.where(i_id == ((p_id & 3) << 5) + (p_id >> 2), 1.0, 0.0)
    fb[...] = jnp.zeros_like(fb)
    sx[pl.ds(x, 1)] = jnp.zeros((1, 8, HD), F32)

    def prepare(part):
        def spread(t, carry):
            slot = lax.broadcasted_iota(jnp.int32, (16, HD), 0) + t * 16
            alive = slot.astype(F32) < table[part, HEADS * RUNS : HEADS * RUNS + 1, :]
            at = pl.ds(pl.multiple_of(part * SLOTS + t * 16, 16), 16)
            for h in range(HEADS):
                bias[h, at, :] = jnp.where(alive, table[part, pl.ds(h * RUNS + t, 1), :], DEAD)
            return carry

        lax.fori_loop(0, RUNS, spread, 0, unroll=4)
        for a in range(2):
            for h in range(HEADS):
                for t in range(SLOTS // CHUNK):
                    rows = slice(part * SLOTS + t * CHUNK, part * SLOTS + (t + 1) * CHUNK)
                    kvt[h, (1 - a) * HD : (2 - a) * HD, rows] = kv[a, rows, h * HD : (h + 1) * HD].T

    prepare(0)
    for copy in swaps:
        copy.wait_recv()
    prepare(1)

    chunks = [slice(t * CHUNK, (t + 1) * CHUNK) for t in range(BOTH // CHUNK)]

    def rows_of(a, h):
        return gat[h, a].reshape(ROWS, HD)

    def forward(h):
        cols = slice(h * HD, (h + 1) * HD)
        queries = rows_of(0, h)
        peak = jnp.full((1, HD), DEAD, F32)
        for rows in chunks:
            score = dot_nt(kv[0, rows, cols], queries) * SCALE + bias[h, rows, :]
            w32[h, rows, :] = score
            peak = jnp.maximum(peak, jnp.max(score, axis=0, keepdims=True))
        total = jnp.zeros((1, HD), F32)
        for rows in chunks:
            weight = jnp.exp(w32[h, rows, :] - peak)
            w32[h, rows, :] = weight
            w16[h, rows, :] = weight.astype(BF16)
            total = total + jnp.sum(weight, axis=0, keepdims=True)
        inverse = 1.0 / total
        mixed = dot(kvt[h], w16[h]) * inverse
        grads = rows_of(1, h).T.astype(F32)
        mean = jnp.sum(mixed[0:HD] * grads, axis=0, keepdims=True)
        mx[h : h + 1, :] = peak
        sx[pl.ds(x, 1), h : h + 1, :] = (peak + jnp.log(total)).reshape(1, 1, HD)
        sx[pl.ds(x, 1), 4 + h : 5 + h, :] = mean.reshape(1, 1, HD)
        return mixed.astype(BF16), mean, inverse

    def shares(h, kept):
        cols = slice(h * HD, (h + 1) * HD)
        mixed, mean, inverse = kept
        grads = rows_of(1, h)
        for rows in chunks:
            dprob = dot_nt(kv[1, rows, cols], grads)
            dp[h, rows, :] = dprob
            dsb[h, rows, :] = (w32[h, rows, :] * (dprob - mean)).astype(BF16)
        slope = (dot(kvt[h, HD : 2 * HD, :], dsb[h]) * inverse).astype(BF16)
        turned = jnp.concatenate([mixed, slope], axis=0)
        sf[h] = dot_nt(perm[...].astype(BF16), turned).astype(BF16).reshape(4, 32, COLS)
        for d in (2, 1, 3):
            remote(
                sf.at[h, xs_of[d]], rx.at[h, x], fsend.at[0], frecv.at[h],
                (q, ctx_of(xs_of[d], zl, k)),
            ).start()

    def await_recv(ref, sem):
        remote(ref, ref, sem, sem, partner).wait_recv()

    def await_send(ref, sem):
        remote(ref, ref, sem, sem, partner).wait_send()

    for h in range(HEADS):
        @pl.when(first)
        def _():
            await_recv(gat.at[h, :, 0:3], brecv.at[h])

        @pl.when(second)
        def _():
            await_recv(gat.at[h], brecv.at[h])

        kept = forward(h)
        if h == HEADS - 1:
            for d in (2, 1, 3):
                remote(
                    sx.at[x], sx.at[x], xsend.at[0], xrecv.at[0], (q, ctx_of(xs_of[d], zl, k))
                ).start()
        shares(h, kept)

    def merge(parts):
        logs, means = parts[:, 0:4, :], parts[:, 4:8, :]
        top = jnp.max(logs, axis=0)
        share = jnp.exp(logs - top[None])
        whole = jnp.sum(share, axis=0)
        return top + jnp.log(whole), jnp.sum(share * means, axis=0) / whole

    await_recv(sx.at[0:3], xrecv.at[0])
    logs, means = merge(sx[...])
    sz[pl.ds(zl, 1), 0:4, :] = logs[None]
    sz[pl.ds(zl, 1), 4:8, :] = means[None]
    for d in (2, 1, 3):
        remote(
            sz.at[zl], sz.at[zl], zsend.at[0], zrecv.at[0], (q, ctx_of(x, zs[d], k))
        ).start()
    own_rows = lax.broadcasted_iota(jnp.int32, (32, HD), 0) + x * 32
    own_lane = ((own_rows & 3) << 5) + (own_rows >> 2)
    pick = jnp.where(lax.broadcasted_iota(jnp.int32, (32, HD), 1) == own_lane, 1.0, 0.0)
    await_recv(sz.at[0:3], zrecv.at[0])
    log_total, delta = merge(sz[...])
    gain = jnp.exp(sx[:, 0:4, :] - log_total[None])
    tilt = gain * (sx[:, 4:8, :] - delta[None])
    both = jnp.concatenate([gain, tilt], axis=1).reshape(32, HD)
    columns = lax.dot_general(
        pick, both, NT, preferred_element_type=F32, precision=lax.Precision.HIGHEST
    )

    for h in range(HEADS):
        rx[h, pl.ds(x, 1)] = sf[h, pl.ds(x, 1)]
        await_recv(rx.at[h, 0:3], frecv.at[h])
        attn_rows = jnp.zeros((32, HD), F32)
        grad_rows = jnp.zeros((32, HD), F32)
        for s in range(4):
            gain_s = columns[:, s * 8 + h : s * 8 + h + 1]
            tilt_s = columns[:, s * 8 + 4 + h : s * 8 + 5 + h]
            part = rx[h, s].astype(F32)
            attn_rows = attn_rows + gain_s * part[:, 0:HD]
            grad_rows = grad_rows + (tilt_s * part[:, HD : 2 * HD] + gain_s * part[:, 2 * HD :])
        fb[pl.ds(h, 32, stride=8), :] = attn_rows
        fb[pl.ds(HEADS + h, 32, stride=8), :] = grad_rows * SCALE
    sy[...] = fb[...].astype(BF16).reshape(32, 8, HD)

    me = zl * 8 + q

    def row_send(dz, dy, dk):
        kp = lax.rem(k + dk, 2)
        remote(
            sy.at[zs[dz] * 8 + kp * 4 + ys[dy]], ry.at[me], ysend.at[0], yrecv.at[0],
            (ys[dy] * 2 + lax.rem(zh + k, 2), ctx_of(x, zs[dz], kp)),
        ).start()

    for dz in (2, 1, 3, 0):
        for dy in (2, 1, 3, 0):
            for dk in (1, 0):
                if dz or dy or dk:
                    row_send(dz, dy, dk)

    @pl.when(second)
    def _():
        row_send(0, 0, 0)

    @pl.when(first)
    def _():
        ry[pl.ds(me, 1)] = sy[pl.ds(zl * 8 + y, 1)]

    for h in range(HEADS):
        cols = slice(h * HD, (h + 1) * HD)
        factor = jnp.exp(mx[h : h + 1, :] - log_total[h : h + 1])
        center = delta[h : h + 1]
        for rows in chunks[::-1]:
            prob = w32[h, rows, :] * factor
            pb[h, rows, :] = prob.astype(BF16)
            dsb[h, rows, :] = (prob * (dp[h, rows, :] - center)).astype(BF16)
        half = len(chunks) // 2
        for n, rows in enumerate(chunks[half:]):
            xs[h, 0, chunks[n], :] = (dot(dsb[h, rows, :], rows_of(0, h)) * SCALE).astype(BF16)
            xs[h, 1, chunks[n], :] = dot(pb[h, rows, :], rows_of(1, h)).astype(BF16)
        remote(xs.at[h], xr.at[h], gsend.at[0], grecv.at[h], partner).start()
        for rows in chunks[:half]:
            kvo[0, rows, cols] = dot(dsb[h, rows, :], rows_of(0, h)) * SCALE
            kvo[1, rows, cols] = dot(pb[h, rows, :], rows_of(1, h))
    for h in range(HEADS):
        cols = slice(h * HD, (h + 1) * HD)
        await_recv(xr.at[h], grecv.at[h])
        kg_ref[:, cols] = (kvo[0, :, cols] + xr[h, 0].astype(F32)).astype(BF16)
        vg_ref[:, cols] = (kvo[1, :, cols] + xr[h, 1].astype(F32)).astype(BF16)

    @pl.when(first)
    def _():
        await_recv(ry.at[0:31], yrecv.at[0])

    @pl.when(second)
    def _():
        await_recv(ry, yrecv.at[0])

    final = jnp.sum(ry[...].astype(F32).reshape(4, 8, 8, HD), axis=0)
    for qd in range(8):
        for h in range(HEADS):
            cols = slice((qd * HEADS + h) * HD, (qd * HEADS + h + 1) * HD)
            attn_ref[:, cols] = final[qd, h : h + 1, :].astype(BF16)
            dq_ref[:, cols] = final[qd, HEADS + h : HEADS + h + 1, :].astype(BF16)

    for copy in swaps:
        copy.wait_send()
    await_send(sx.at[0:3], xsend.at[0])
    await_send(sz.at[0:3], zsend.at[0])
    await_send(sf.at[:, 0:3], fsend.at[0])
    await_send(xs, gsend.at[0])

    @pl.when(first)
    def _():
        await_send(gat.at[:, :, 0:3], bsend.at[0])
        await_send(sy.at[0:31], ysend.at[0])

    @pl.when(second)
    def _():
        await_send(sy, ysend.at[0])

    @pl.when(jnp.logical_and(second, edge))
    def _():
        await_send(own, bsend.at[0])


def write_out(attn_in, dq_in, kg_in, vg_in, attn_out, dq_out, kg_out, vg_out, sems):
    pairs = ((kg_in, kg_out), (vg_in, vg_out), (attn_in, attn_out), (dq_in, dq_out))
    copies = [pltpu.make_async_copy(a, b, sems.at[n]) for n, (a, b) in enumerate(pairs)]
    for copy in copies:
        copy.start()
    for copy in copies:
        copy.wait()


def local(query_states, key_states, value_states, level_ids, level_bias, live_counts, out_grad):
    hbm = pl.BlockSpec(memory_space=pltpu.HBM)
    vmem = pl.BlockSpec(memory_space=pltpu.VMEM)
    dma = pltpu.SemaphoreType.DMA
    arrays = (
        query_states, key_states, value_states, level_ids, level_bias, live_counts, out_grad
    )
    shapes = ((1, 3072), (1, 3072), key_states.shape, value_states.shape)
    results = pl.pallas_call(
        kernel,
        name="framepack",
        out_shape=tuple(pltpu.VMEM(shape, BF16) for shape in shapes),
        in_specs=[hbm] * 7,
        out_specs=(vmem,) * 4,
        scratch_shapes=[
            pltpu.VMEM((2, 32, 3072), BF16),
            pltpu.VMEM((HEADS, 2, 4, 32, HD), BF16),
            pltpu.VMEM((2, BOTH, COLS), BF16),
            pltpu.VMEM((HEADS, 2 * HD, BOTH), BF16),
            pltpu.VMEM((2, HEADS * RUNS + 8, HD), F32),
            pltpu.VMEM((HEADS, BOTH, HD), F32),
            pltpu.VMEM((HD, HD), F32),
            pltpu.VMEM((HEADS, BOTH, ROWS), F32),
            pltpu.VMEM((HEADS, BOTH, ROWS), BF16),
            pltpu.VMEM((HEADS, BOTH, ROWS), F32),
            pltpu.VMEM((HEADS, BOTH, ROWS), BF16),
            pltpu.VMEM((HEADS, BOTH, ROWS), BF16),
            pltpu.VMEM((8, ROWS), F32),
            pltpu.VMEM((4, 8, HD), F32),
            pltpu.VMEM((4, 8, HD), F32),
            pltpu.VMEM((HEADS, 4, 32, COLS), BF16),
            pltpu.VMEM((HEADS, 4, 32, COLS), BF16),
            pltpu.VMEM((32 * 8, HD), F32),
            pltpu.VMEM((32, 8, HD), BF16),
            pltpu.VMEM((32, 8, HD), BF16),
            pltpu.VMEM((2, SLOTS, COLS), F32),
            pltpu.VMEM((HEADS, 2, SLOTS, HD), BF16),
            pltpu.VMEM((HEADS, 2, SLOTS, HD), BF16),
            pltpu.SMEM((SLOTS,), jnp.int32),
            pltpu.SMEM((5, 24), F32),
            pltpu.SMEM((1,), jnp.int32),
            dma((7,)),
            dma((3,)), dma((3,)),
            dma((1,)), dma((HEADS,)),
            dma((1,)), dma((1,)),
            dma((1,)), dma((1,)),
            dma((1,)), dma((HEADS,)),
            dma((1,)), dma((1,)),
            dma((1,)), dma((HEADS,)),
        ],
        compiler_params=pltpu.CompilerParams(
            collective_id=0, has_side_effects=True, vmem_limit_bytes=40 * 1024 * 1024
        ),
    )(*(a if a is live_counts else pltpu.with_memory_space_constraint(a, pltpu.HBM) for a in arrays))
    return pl.pallas_call(
        write_out,
        name="write_out",
        out_shape=tuple(jax.ShapeDtypeStruct(shape, BF16) for shape in shapes),
        in_specs=[vmem] * 4,
        out_specs=(hbm,) * 4,
        scratch_shapes=[dma((4,))],
    )(*(pltpu.with_memory_space_constraint(a, pltpu.VMEM) for a in results))


def solution(mesh):
    placed = (
        P("query", None),
        P("ctx", "query"),
        P("ctx", "query"),
        P("ctx"),
        P(),
        P("ctx"),
        P("query", None),
    )
    return jax.shard_map(
        local,
        mesh=mesh,
        in_specs=placed,
        out_specs=(
            P(("query", "ctx"), None),
            P(("query", "ctx"), None),
            P("ctx", "query"),
            P("ctx", "query"),
        ),
        check_vma=False,
    )
```

```python
import math

import jax
import jax.numpy as jnp
from jax import lax
from jax.experimental import pallas as pl
from jax.experimental.pallas import tpu as pltpu
from jax.sharding import PartitionSpec as P

MESH = pl.DeviceIdType.MESH
F32 = jnp.float32
BF16 = jnp.bfloat16
HD = 128
HEADS = 3
COLS = HEADS * HD
ROWS = 128
SLOTS = 1024
BOTH = 2 * SLOTS
RUNS = SLOTS // 16
CHUNK = 256
SCALE = 1.0 / math.sqrt(HD)
NT = (((1,), (1,)), ((), ()))
DEAD = -1e30


def dot_nt(a, b):
    return lax.dot_general(a, b, NT, preferred_element_type=F32)


def dot(a, b):
    return jnp.dot(a, b, preferred_element_type=F32)


def kernel(
    q_hbm, k_hbm, v_hbm, lid_hbm, lb_hbm, lc_hbm, g_hbm,
    attn_ref, dq_ref, kg_ref, vg_ref,
    own, gat, kv, kvt, table, bias, perm, w32, w16, dp, pb, dsb, mx,
    sx, sf, rx, fb, sy, ry, kvo, xs, xr, lid, lb, lc,
    ld, dsend, drecv, bsend, brecv, xsend, xrecv, token,
    fsend, frecv, ysend, yrecv, gsend, grecv,
):
    q = lax.axis_index("query")
    c = lax.axis_index("ctx")
    y, zh = q // 2, q % 2
    x, zl, k = c // 8, (c // 2) % 4, c % 2
    first, second = k == 0, k == 1

    def ctx_of(xx, zz, kk):
        return xx * 8 + zz * 2 + kk

    def load(src, dst, n):
        copy = pltpu.make_async_copy(src, dst, ld.at[n])
        copy.start()
        return copy

    loads = [
        load(q_hbm, own.at[0], 0),
        load(g_hbm, own.at[1], 1),
        load(lid_hbm, lid, 2),
        load(lb_hbm, lb, 3),
        load(lc_hbm, lc, 4),
        load(k_hbm, kv.at[0, 0:SLOTS], 5),
        load(v_hbm, kv.at[1, 0:SLOTS], 6),
    ]

    edge = zl % 3 == 0
    near, far = 3 - zl, 2 - zl // 3
    partner = (q, ctx_of(x, zl, 1 - k))
    ys = [lax.rem(y + d, 4) for d in range(4)]
    xs_of = [lax.rem(x + d, 4) for d in range(4)]
    zs = [lax.rem(zl + d, 4) for d in range(4)]
    barrier = pltpu.get_barrier_semaphore()

    def greet(device):
        pl.semaphore_signal(barrier, inc=1, device_id=device, device_id_type=MESH)

    for d in range(1, 4):
        greet((q, ctx_of(x, zs[d], 0)))
        greet((q, ctx_of(x, zs[d], 1)))
        greet((q, ctx_of(xs_of[d], zl, k)))
    greet(partner)

    @pl.when(first)
    def _():
        for d in range(1, 4):
            greet((ys[d] * 2 + zh, c))
        pl.semaphore_wait(barrier, 13)

    @pl.when(jnp.logical_and(second, edge))
    def _():
        for d in range(4):
            greet((ys[d] * 2 + 1 - zh, ctx_of(x, near, 1)))
            greet((ys[d] * 2 + 1 - zh, ctx_of(x, far, 1)))
        pl.semaphore_wait(barrier, 18)

    @pl.when(jnp.logical_and(second, jnp.logical_not(edge)))
    def _():
        for d in range(4):
            greet((ys[d] * 2 + 1 - zh, ctx_of(x, jnp.where(zl < 2, 3, 0), 1)))
        pl.semaphore_wait(barrier, 14)

    for d in range(1, 4):
        pl.semaphore_signal(
            token, inc=1, device_id=(q, ctx_of(xs_of[d], zl, k)), device_id_type=MESH
        )

    loads[0].wait()
    loads[1].wait()

    def remote(src, dst, send, recv, device):
        return pltpu.make_async_remote_copy(
            src_ref=src, dst_ref=dst, send_sem=send, recv_sem=recv,
            device_id=device, device_id_type=MESH,
        )

    def block_send(h, yd, half, zz):
        qd = yd * 2 + half
        cols = pl.ds(pl.multiple_of(qd * COLS + h * HD, HD), HD)
        remote(
            own.at[:, :, cols], gat.at[h, :, y], bsend.at[0], brecv.at[h, y],
            (qd, ctx_of(x, zz, k)),
        ).start()

    @pl.when(first)
    def _():
        for h in range(HEADS):
            for d in (2, 1, 3):
                block_send(h, ys[d], zh, zl)
            cols = pl.ds(pl.multiple_of(q * COLS + h * HD, HD), HD)
            gat[h, :, pl.ds(y, 1)] = own[:, :, cols].reshape(2, 1, 32, HD)

    @pl.when(jnp.logical_and(second, edge))
    def _():
        for h in range(HEADS):
            for d in (2, 1, 3, 0):
                block_send(h, ys[d], 1 - zh, far)
                block_send(h, ys[d], 1 - zh, near)

    loads[2].wait()
    loads[3].wait()
    loads[4].wait()

    def fill(t, carry):
        level = lid[t * 16]
        for h in range(HEADS):
            table[0, pl.ds(h * RUNS + t, 1), :] = jnp.full((1, HD), lb[level, q * HEADS + h], F32)
        return carry

    lax.fori_loop(0, RUNS, fill, 0)
    table[0, HEADS * RUNS :, :] = jnp.full((8, HD), lc[0].astype(F32), F32)
    loads[5].wait()
    loads[6].wait()
    swaps = [
        remote(table.at[0], table.at[1], dsend.at[0], drecv.at[0], partner),
        remote(kv.at[0, 0:SLOTS], kv.at[0, SLOTS:BOTH], dsend.at[1], drecv.at[1], partner),
        remote(kv.at[1, 0:SLOTS], kv.at[1, SLOTS:BOTH], dsend.at[2], drecv.at[2], partner),
    ]
    for copy in swaps:
        copy.start()

    p_id = lax.broadcasted_iota(jnp.int32, (HD, HD), 0)
    i_id = lax.broadcasted_iota(jnp.int32, (HD, HD), 1)
    perm[...] = jnp.where(i_id == ((p_id & 3) << 5) + (p_id >> 2), 1.0, 0.0)
    fb[...] = jnp.zeros_like(fb)
    here = zl * 4 + x
    sx[pl.ds(here, 1)] = jnp.zeros((1, 8, HD), F32)

    def prepare(part):
        def spread(t, carry):
            slot = lax.broadcasted_iota(jnp.int32, (16, HD), 0) + t * 16
            alive = slot.astype(F32) < table[part, HEADS * RUNS : HEADS * RUNS + 1, :]
            at = pl.ds(pl.multiple_of(part * SLOTS + t * 16, 16), 16)
            for h in range(HEADS):
                bias[h, at, :] = jnp.where(alive, table[part, pl.ds(h * RUNS + t, 1), :], DEAD)
            return carry

        lax.fori_loop(0, RUNS, spread, 0, unroll=4)
        for a in range(2):
            for h in range(HEADS):
                for t in range(SLOTS // CHUNK):
                    rows = slice(part * SLOTS + t * CHUNK, part * SLOTS + (t + 1) * CHUNK)
                    kvt[h, (1 - a) * HD : (2 - a) * HD, rows] = kv[a, rows, h * HD : (h + 1) * HD].T

    prepare(0)
    for copy in swaps:
        copy.wait_recv()
    prepare(1)

    chunks = [slice(t * CHUNK, (t + 1) * CHUNK) for t in range(BOTH // CHUNK)]

    def rows_of(a, h):
        return gat[h, a].reshape(ROWS, HD)

    def forward(h):
        cols = slice(h * HD, (h + 1) * HD)
        queries = rows_of(0, h)
        peak = jnp.full((1, HD), DEAD, F32)
        for rows in chunks:
            score = dot_nt(kv[0, rows, cols], queries) * SCALE + bias[h, rows, :]
            w32[h, rows, :] = score
            peak = jnp.maximum(peak, jnp.max(score, axis=0, keepdims=True))
        total = jnp.zeros((1, HD), F32)
        for rows in chunks:
            weight = jnp.exp(w32[h, rows, :] - peak)
            w32[h, rows, :] = weight
            w16[h, rows, :] = weight.astype(BF16)
            total = total + jnp.sum(weight, axis=0, keepdims=True)
        inverse = 1.0 / total
        mixed = dot(kvt[h], w16[h]) * inverse
        grads = rows_of(1, h).T.astype(F32)
        mean = jnp.sum(mixed[0:HD] * grads, axis=0, keepdims=True)
        mx[h : h + 1, :] = peak
        sx[pl.ds(here, 1), h : h + 1, :] = (peak + jnp.log(total)).reshape(1, 1, HD)
        sx[pl.ds(here, 1), 4 + h : 5 + h, :] = mean.reshape(1, 1, HD)
        return mixed.astype(BF16), mean, inverse

    def shares(h, kept):
        cols = slice(h * HD, (h + 1) * HD)
        mixed, mean, inverse = kept
        grads = rows_of(1, h)
        for rows in chunks:
            dprob = dot_nt(kv[1, rows, cols], grads)
            dp[h, rows, :] = dprob
            dsb[h, rows, :] = (w32[h, rows, :] * (dprob - mean)).astype(BF16)
        slope = (dot(kvt[h, HD : 2 * HD, :], dsb[h]) * inverse).astype(BF16)
        turned = jnp.concatenate([mixed, slope], axis=0)
        sf[h] = dot_nt(perm[...].astype(BF16), turned).astype(BF16).reshape(4, 32, COLS)
        for d in (2, 1, 3):
            remote(
                sf.at[h, xs_of[d]], rx.at[h, x], fsend.at[0], frecv.at[h],
                (q, ctx_of(xs_of[d], zl, k)),
            ).start()

    def await_recv(ref, sem):
        remote(ref, ref, sem, sem, partner).wait_recv()

    def await_send(ref, sem):
        remote(ref, ref, sem, sem, partner).wait_send()

    kept = []
    for h in range(HEADS):
        @pl.when(first)
        def _():
            for d in (1, 3, 2):
                await_recv(gat.at[h, :, ys[d]], brecv.at[h, ys[d]])

        @pl.when(second)
        def _():
            for d in (2, 3, 1, 0):
                await_recv(gat.at[h, :, ys[d]], brecv.at[h, ys[d]])

        kept.append(forward(h))
        if h < 2:
            shares(h, kept[h])
    pl.semaphore_wait(token, 3)
    for dz in (2, 1, 3, 0):
        for dx in (2, 1, 3, 0):
            if dz or dx:
                remote(
                    sx.at[here], sx.at[here], xsend.at[0], xrecv.at[0],
                    (q, ctx_of(xs_of[dx], zs[dz], k)),
                ).start()
    shares(2, kept[2])

    def merge(parts):
        logs, means = parts[:, 0:4, :], parts[:, 4:8, :]
        top = jnp.max(logs, axis=0)
        share = jnp.exp(logs - top[None])
        whole = jnp.sum(share, axis=0)
        return top + jnp.log(whole), jnp.sum(share * means, axis=0) / whole

    own_rows = lax.broadcasted_iota(jnp.int32, (32, HD), 0) + x * 32
    own_lane = ((own_rows & 3) << 5) + (own_rows >> 2)
    pick = jnp.where(lax.broadcasted_iota(jnp.int32, (32, HD), 1) == own_lane, 1.0, 0.0)

    def columns_of(gain, tilt, n):
        both = jnp.concatenate([gain, tilt], axis=-2).reshape(n * 8, HD)
        return lax.dot_general(
            pick, both, NT, preferred_element_type=F32, precision=lax.Precision.HIGHEST
        )

    for h in range(HEADS):
        rx[h, pl.ds(x, 1)] = sf[h, pl.ds(x, 1)]
        await_recv(rx.at[h, 0:3], frecv.at[h])
    await_recv(sx.at[0:15], xrecv.at[0])
    log_total, delta = merge(sx[...])
    row = sx[pl.ds(zl * 4, 4)]
    gain = jnp.exp(row[:, 0:4, :] - log_total[None])
    columns = columns_of(gain, gain * (row[:, 4:8, :] - delta[None]), 4)
    for h in range(HEADS):
        attn_rows = jnp.zeros((32, HD), F32)
        grad_rows = jnp.zeros((32, HD), F32)
        for s in range(4):
            gain_s = columns[:, s * 8 + h : s * 8 + h + 1]
            tilt_s = columns[:, s * 8 + 4 + h : s * 8 + 5 + h]
            part = rx[h, s].astype(F32)
            attn_rows = attn_rows + gain_s * part[:, 0:HD]
            grad_rows = grad_rows + (tilt_s * part[:, HD : 2 * HD] + gain_s * part[:, 2 * HD :])
        fb[pl.ds(h, 32, stride=8), :] = attn_rows
        fb[pl.ds(HEADS + h, 32, stride=8), :] = grad_rows * SCALE
    sy[...] = fb[...].astype(BF16).reshape(32, 8, HD)

    me = zl * 8 + q

    def row_send(dz, dy, dk):
        kp = lax.rem(k + dk, 2)
        remote(
            sy.at[zs[dz] * 8 + kp * 4 + ys[dy]], ry.at[me], ysend.at[0], yrecv.at[0],
            (ys[dy] * 2 + lax.rem(zh + k, 2), ctx_of(x, zs[dz], kp)),
        ).start()

    for dy in (2, 1, 3, 0):
        for dz in (0, 1, 3, 2):
            for dk in (1, 0):
                if dz or dy or dk:
                    row_send(dz, dy, dk)
        if dy == 1:
            @pl.when(second)
            def _():
                row_send(0, 0, 0)

    @pl.when(first)
    def _():
        ry[pl.ds(me, 1)] = sy[pl.ds(zl * 8 + y, 1)]

    for h in range(HEADS):
        cols = slice(h * HD, (h + 1) * HD)
        factor = jnp.exp(mx[h : h + 1, :] - log_total[h : h + 1])
        center = delta[h : h + 1]
        for rows in chunks[::-1]:
            prob = w32[h, rows, :] * factor
            pb[h, rows, :] = prob.astype(BF16)
            dsb[h, rows, :] = (prob * (dp[h, rows, :] - center)).astype(BF16)
        half = len(chunks) // 2
        for n, rows in enumerate(chunks[half:]):
            xs[h, 0, chunks[n], :] = (dot(dsb[h, rows, :], rows_of(0, h)) * SCALE).astype(BF16)
            xs[h, 1, chunks[n], :] = dot(pb[h, rows, :], rows_of(1, h)).astype(BF16)
        remote(xs.at[h], xr.at[h], gsend.at[0], grecv.at[h], partner).start()
        for rows in chunks[:half]:
            kvo[0, rows, cols] = dot(dsb[h, rows, :], rows_of(0, h)) * SCALE
            kvo[1, rows, cols] = dot(pb[h, rows, :], rows_of(1, h))
    for h in range(HEADS):
        cols = slice(h * HD, (h + 1) * HD)
        await_recv(xr.at[h], grecv.at[h])
        kg_ref[:, cols] = (kvo[0, :, cols] + xr[h, 0].astype(F32)).astype(BF16)
        vg_ref[:, cols] = (kvo[1, :, cols] + xr[h, 1].astype(F32)).astype(BF16)

    @pl.when(first)
    def _():
        await_recv(ry.at[0:31], yrecv.at[0])

    @pl.when(second)
    def _():
        await_recv(ry, yrecv.at[0])

    final = jnp.sum(ry[...].astype(F32).reshape(4, 8, 8, HD), axis=0)
    for qd in range(8):
        for h in range(HEADS):
            cols = slice((qd * HEADS + h) * HD, (qd * HEADS + h + 1) * HD)
            attn_ref[:, cols] = final[qd, h : h + 1, :].astype(BF16)
            dq_ref[:, cols] = final[qd, HEADS + h : HEADS + h + 1, :].astype(BF16)

    for copy in swaps:
        copy.wait_send()
    await_send(sx.at[0:15], xsend.at[0])
    await_send(sf.at[:, 0:3], fsend.at[0])
    await_send(xs, gsend.at[0])

    @pl.when(first)
    def _():
        await_send(gat.at[:, :, 0:3], bsend.at[0])
        await_send(sy.at[0:31], ysend.at[0])

    @pl.when(second)
    def _():
        await_send(sy, ysend.at[0])

    @pl.when(jnp.logical_and(second, edge))
    def _():
        await_send(own, bsend.at[0])


def write_out(attn_in, dq_in, kg_in, vg_in, attn_out, dq_out, kg_out, vg_out, sems):
    pairs = [(attn_in, attn_out), (dq_in, dq_out)]
    for t in range(SLOTS // CHUNK):
        rows = pl.ds(t * CHUNK, CHUNK)
        pairs += [(kg_in.at[rows], kg_out.at[rows]), (vg_in.at[rows], vg_out.at[rows])]
    copies = [pltpu.make_async_copy(a, b, sems.at[n]) for n, (a, b) in enumerate(pairs)]
    for copy in copies:
        copy.start()
    for copy in copies:
        copy.wait()


def local(query_states, key_states, value_states, level_ids, level_bias, live_counts, out_grad):
    hbm = pl.BlockSpec(memory_space=pltpu.HBM)
    vmem = pl.BlockSpec(memory_space=pltpu.VMEM)
    dma = pltpu.SemaphoreType.DMA
    arrays = (
        query_states, key_states, value_states, level_ids, level_bias, live_counts, out_grad
    )
    shapes = ((1, 3072), (1, 3072), key_states.shape, value_states.shape)
    results = pl.pallas_call(
        kernel,
        name="framepack",
        out_shape=tuple(pltpu.VMEM(shape, BF16) for shape in shapes),
        in_specs=[hbm] * 5 + [pl.BlockSpec(memory_space=pl.ANY), hbm],
        out_specs=(vmem,) * 4,
        scratch_shapes=[
            pltpu.VMEM((2, 32, 3072), BF16),
            pltpu.VMEM((HEADS, 2, 4, 32, HD), BF16),
            pltpu.VMEM((2, BOTH, COLS), BF16),
            pltpu.VMEM((HEADS, 2 * HD, BOTH), BF16),
            pltpu.VMEM((2, HEADS * RUNS + 8, HD), F32),
            pltpu.VMEM((HEADS, BOTH, HD), F32),
            pltpu.VMEM((HD, HD), F32),
            pltpu.VMEM((HEADS, BOTH, ROWS), F32),
            pltpu.VMEM((HEADS, BOTH, ROWS), BF16),
            pltpu.VMEM((HEADS, BOTH, ROWS), F32),
            pltpu.VMEM((HEADS, BOTH, ROWS), BF16),
            pltpu.VMEM((HEADS, BOTH, ROWS), BF16),
            pltpu.VMEM((8, ROWS), F32),
            pltpu.VMEM((16, 8, HD), F32),
            pltpu.VMEM((HEADS, 4, 32, COLS), BF16),
            pltpu.VMEM((HEADS, 4, 32, COLS), BF16),
            pltpu.VMEM((32 * 8, HD), F32),
            pltpu.VMEM((32, 8, HD), BF16),
            pltpu.VMEM((32, 8, HD), BF16),
            pltpu.VMEM((2, SLOTS, COLS), F32),
            pltpu.VMEM((HEADS, 2, SLOTS, HD), BF16),
            pltpu.VMEM((HEADS, 2, SLOTS, HD), BF16),
            pltpu.SMEM((SLOTS,), jnp.int32),
            pltpu.SMEM((5, 24), F32),
            pltpu.SMEM((1,), jnp.int32),
            dma((7,)),
            dma((3,)), dma((3,)),
            dma((1,)), dma((HEADS, 4)),
            dma((1,)), dma((1,)),
            pltpu.SemaphoreType.REGULAR,
            dma((1,)), dma((HEADS,)),
            dma((1,)), dma((1,)),
            dma((1,)), dma((HEADS,)),
        ],
        compiler_params=pltpu.CompilerParams(
            collective_id=0, has_side_effects=True, vmem_limit_bytes=40 * 1024 * 1024
        ),
    )(*(a if a is live_counts else pltpu.with_memory_space_constraint(a, pltpu.HBM) for a in arrays))
    return pl.pallas_call(
        write_out,
        name="write_out",
        out_shape=tuple(jax.ShapeDtypeStruct(shape, BF16) for shape in shapes),
        in_specs=[vmem] * 4,
        out_specs=(hbm,) * 4,
        scratch_shapes=[dma((2 + 2 * (SLOTS // CHUNK),))],
    )(*(pltpu.with_memory_space_constraint(a, pltpu.VMEM) for a in results))


def solution(mesh):
    placed = (
        P("query", None),
        P("ctx", "query"),
        P("ctx", "query"),
        P("ctx"),
        P(),
        P("ctx"),
        P("query", None),
    )
    return jax.shard_map(
        local,
        mesh=mesh,
        in_specs=placed,
        out_specs=(
            P(("query", "ctx"), None),
            P(("query", "ctx"), None),
            P("ctx", "query"),
            P("ctx", "query"),
        ),
        check_vma=False,
    )
```

```python
import math

import jax
import jax.numpy as jnp
from jax import lax
from jax.experimental import pallas as pl
from jax.experimental.pallas import tpu as pltpu
from jax.sharding import PartitionSpec as P

MESH = pl.DeviceIdType.MESH
F32 = jnp.float32
BF16 = jnp.bfloat16
HD = 128
HEADS = 3
COLS = HEADS * HD
ROWS = 128
SLOTS = 1024
BOTH = 2 * SLOTS
RUNS = SLOTS // 16
CHUNK = 256
SCALE = 1.0 / math.sqrt(HD)
NT = (((1,), (1,)), ((), ()))
DEAD = -1e30
LOG2E = math.log2(math.e)


def dot_nt(a, b):
    return lax.dot_general(a, b, NT, preferred_element_type=F32)


def dot(a, b):
    return jnp.dot(a, b, preferred_element_type=F32)


def kernel(
    q_hbm, k_hbm, v_hbm, lid_hbm, lb_hbm, lc_hbm, g_hbm,
    attn_ref, dq_ref, kg_ref, vg_ref,
    own, gat, kv, kvt, table, bias, perm, work, w16, dp, pb, dsb, mx,
    sx, sf, rx, fb, sy, ry, kvo, xs, xr, lid, lb, lc,
    ld, dsend, drecv, bsend, brecv, xsend, xrecv, token,
    fsend, frecv, ysend, yrecv, gsend, grecv,
):
    q = lax.axis_index("query")
    c = lax.axis_index("ctx")
    y, zh = q // 2, q % 2
    x, zl, k = c // 8, (c // 2) % 4, c % 2
    first, second = k == 0, k == 1

    def ctx_of(xx, zz, kk):
        return xx * 8 + zz * 2 + kk

    def load(src, dst, n):
        copy = pltpu.make_async_copy(src, dst, ld.at[n])
        copy.start()
        return copy

    loads = [
        load(q_hbm, own.at[0], 0),
        load(g_hbm, own.at[1], 1),
        load(lid_hbm, lid, 2),
        load(lb_hbm, lb, 3),
        load(lc_hbm, lc, 4),
        load(k_hbm, kv.at[0, 0:SLOTS], 5),
        load(v_hbm, kv.at[1, 0:SLOTS], 6),
    ]

    edge = zl % 3 == 0
    near, far = 3 - zl, 2 - zl // 3
    partner = (q, ctx_of(x, zl, 1 - k))
    ys = [lax.rem(y + d, 4) for d in range(4)]
    xs_of = [lax.rem(x + d, 4) for d in range(4)]
    zs = [lax.rem(zl + d, 4) for d in range(4)]
    barrier = pltpu.get_barrier_semaphore()

    def greet(device):
        pl.semaphore_signal(barrier, inc=1, device_id=device, device_id_type=MESH)

    for d in range(1, 4):
        greet((q, ctx_of(x, zs[d], 0)))
        greet((q, ctx_of(x, zs[d], 1)))
        greet((q, ctx_of(xs_of[d], zl, k)))
    greet(partner)

    @pl.when(first)
    def _():
        for d in range(1, 4):
            greet((ys[d] * 2 + zh, c))
        pl.semaphore_wait(barrier, 13)

    @pl.when(jnp.logical_and(second, edge))
    def _():
        for d in range(4):
            greet((ys[d] * 2 + 1 - zh, ctx_of(x, near, 1)))
            greet((ys[d] * 2 + 1 - zh, ctx_of(x, far, 1)))
        pl.semaphore_wait(barrier, 18)

    @pl.when(jnp.logical_and(second, jnp.logical_not(edge)))
    def _():
        for d in range(4):
            greet((ys[d] * 2 + 1 - zh, ctx_of(x, jnp.where(zl < 2, 3, 0), 1)))
        pl.semaphore_wait(barrier, 14)

    for d in range(1, 4):
        pl.semaphore_signal(
            token, inc=1, device_id=(q, ctx_of(xs_of[d], zl, k)), device_id_type=MESH
        )

    loads[0].wait()
    loads[1].wait()

    def remote(src, dst, send, recv, device):
        return pltpu.make_async_remote_copy(
            src_ref=src, dst_ref=dst, send_sem=send, recv_sem=recv,
            device_id=device, device_id_type=MESH,
        )

    def block_send(h, yd, half, zz):
        qd = yd * 2 + half
        cols = pl.ds(pl.multiple_of(qd * COLS + h * HD, HD), HD)
        remote(
            own.at[:, :, cols], gat.at[h, :, y], bsend.at[0], brecv.at[h],
            (qd, ctx_of(x, zz, k)),
        ).start()

    @pl.when(first)
    def _():
        for h in range(HEADS):
            for d in (2, 1, 3):
                block_send(h, ys[d], zh, zl)
            cols = pl.ds(pl.multiple_of(q * COLS + h * HD, HD), HD)
            gat[h, :, pl.ds(y, 1)] = own[:, :, cols].reshape(2, 1, 32, HD)

    @pl.when(jnp.logical_and(second, edge))
    def _():
        for h in range(HEADS):
            for d in (2, 1, 3, 0):
                block_send(h, ys[d], 1 - zh, far)
                block_send(h, ys[d], 1 - zh, near)

    loads[2].wait()
    loads[3].wait()
    loads[4].wait()

    def fill(t, carry):
        level = lid[t * 16]
        for h in range(HEADS):
            table[0, pl.ds(h * RUNS + t, 1), :] = jnp.full(
                (1, HD), lb[level, q * HEADS + h] * LOG2E, F32
            )
        return carry

    lax.fori_loop(0, RUNS, fill, 0)
    table[0, HEADS * RUNS :, :] = jnp.full((8, HD), lc[0].astype(F32), F32)
    loads[5].wait()
    loads[6].wait()
    swaps = [
        remote(table.at[0], table.at[1], dsend.at[0], drecv.at[0], partner),
        remote(kv.at[0, 0:SLOTS], kv.at[0, SLOTS:BOTH], dsend.at[1], drecv.at[1], partner),
        remote(kv.at[1, 0:SLOTS], kv.at[1, SLOTS:BOTH], dsend.at[2], drecv.at[2], partner),
    ]
    for copy in swaps:
        copy.start()

    p_id = lax.broadcasted_iota(jnp.int32, (HD, HD), 0)
    i_id = lax.broadcasted_iota(jnp.int32, (HD, HD), 1)
    perm[...] = jnp.where(i_id == ((p_id & 3) << 5) + (p_id >> 2), 1.0, 0.0)
    fb[...] = jnp.zeros_like(fb)
    here = zl * 4 + x
    sx[pl.ds(here, 1)] = jnp.zeros((1, 8, HD), F32)

    def prepare(part):
        def spread(t, carry):
            slot = lax.broadcasted_iota(jnp.int32, (16, HD), 0) + t * 16
            alive = slot.astype(F32) < table[part, HEADS * RUNS : HEADS * RUNS + 1, :]
            at = pl.ds(pl.multiple_of(part * SLOTS + t * 16, 16), 16)
            for h in range(HEADS):
                bias[h, at, :] = jnp.where(alive, table[part, pl.ds(h * RUNS + t, 1), :], DEAD)
            return carry

        lax.fori_loop(0, RUNS, spread, 0, unroll=4)
        for a in range(2):
            for h in range(HEADS):
                for t in range(SLOTS // CHUNK):
                    rows = slice(part * SLOTS + t * CHUNK, part * SLOTS + (t + 1) * CHUNK)
                    kvt[h, (1 - a) * HD : (2 - a) * HD, rows] = kv[a, rows, h * HD : (h + 1) * HD].T

    prepare(0)
    for copy in swaps:
        copy.wait_recv()
    prepare(1)

    chunks = [slice(t * CHUNK, (t + 1) * CHUNK) for t in range(BOTH // CHUNK)]

    def rows_of(a, h):
        return gat[h, a].reshape(ROWS, HD)

    def forward(h):
        cols = slice(h * HD, (h + 1) * HD)
        queries = rows_of(0, h)
        peak = jnp.full((1, HD), DEAD, F32)
        for rows in chunks:
            score = dot_nt(kv[0, rows, cols], queries) * (SCALE * LOG2E) + bias[h, rows, :]
            work[rows, :] = score
            peak = jnp.maximum(peak, jnp.max(score, axis=0, keepdims=True))
        total = jnp.zeros((1, HD), F32)
        for rows in chunks:
            weight = jnp.exp2(work[rows, :] - peak)
            w16[h, rows, :] = weight.astype(BF16)
            total = total + jnp.sum(weight, axis=0, keepdims=True)
        inverse = 1.0 / total
        mixed = dot(kvt[h], w16[h]) * inverse
        grads = rows_of(1, h).T.astype(F32)
        mean = jnp.sum(mixed[0:HD] * grads, axis=0, keepdims=True)
        peak = peak * (1.0 / LOG2E)
        mx[h : h + 1, :] = peak
        sx[pl.ds(here, 1), h : h + 1, :] = (peak + jnp.log(total)).reshape(1, 1, HD)
        sx[pl.ds(here, 1), 4 + h : 5 + h, :] = mean.reshape(1, 1, HD)
        return mixed.astype(BF16), mean, inverse

    def send_shares(h):
        for d in (2, 1, 3):
            remote(
                sf.at[h, xs_of[d]], rx.at[h, x], fsend.at[0], frecv.at[h],
                (q, ctx_of(xs_of[d], zl, k)),
            ).start()

    def shares(h, kept):
        cols = slice(h * HD, (h + 1) * HD)
        mixed, mean, inverse = kept
        turn = perm[...].astype(BF16)
        grads = rows_of(1, h)
        for rows in chunks:
            dprob = dot_nt(kv[1, rows, cols], grads)
            dp[h, rows, :] = dprob
            dsb[h, rows, :] = (w16[h, rows, :].astype(F32) * (dprob - mean)).astype(BF16)
        slope = (dot(kvt[h, HD : 2 * HD, :], dsb[h]) * inverse).astype(BF16)
        turned = jnp.concatenate([mixed, slope], axis=0)
        sf[h] = dot_nt(turn, turned).astype(BF16).reshape(4, 32, COLS)
        send_shares(h)

    def await_recv(ref, sem):
        remote(ref, ref, sem, sem, partner).wait_recv()

    def await_send(ref, sem):
        remote(ref, ref, sem, sem, partner).wait_send()

    kept = []
    for h in range(HEADS):
        @pl.when(first)
        def _():
            await_recv(gat.at[h, :, 0:3], brecv.at[h])

        @pl.when(second)
        def _():
            await_recv(gat.at[h], brecv.at[h])

        kept.append(forward(h))
        if h < 2:
            shares(h, kept[h])
    pl.semaphore_wait(token, 3)
    for dx in (2, 1, 3, 0):
        for dz in (2, 1, 3, 0):
            if dz or dx:
                remote(
                    sx.at[here], sx.at[here], xsend.at[0], xrecv.at[0],
                    (q, ctx_of(xs_of[dx], zs[dz], k)),
                ).start()
    shares(2, kept[2])

    def merge(parts):
        logs, means = parts[:, 0:4, :], parts[:, 4:8, :]
        top = jnp.max(logs, axis=0)
        share = jnp.exp(logs - top[None])
        whole = jnp.sum(share, axis=0)
        return top + jnp.log(whole), jnp.sum(share * means, axis=0) / whole

    own_rows = lax.broadcasted_iota(jnp.int32, (32, HD), 0) + x * 32
    own_lane = ((own_rows & 3) << 5) + (own_rows >> 2)
    pick = jnp.where(lax.broadcasted_iota(jnp.int32, (32, HD), 1) == own_lane, 1.0, 0.0)

    def columns_of(gain, tilt, n):
        both = jnp.concatenate([gain, tilt], axis=-2).reshape(n * 8, HD)
        return lax.dot_general(
            pick, both, NT, preferred_element_type=F32, precision=lax.Precision.HIGHEST
        )

    for h in range(HEADS):
        rx[h, pl.ds(x, 1)] = sf[h, pl.ds(x, 1)]
        await_recv(rx.at[h, 0:3], frecv.at[h])
    await_recv(sx.at[0:15], xrecv.at[0])
    log_total, delta = merge(sx[...])
    row = sx[pl.ds(zl * 4, 4)]
    gain = jnp.exp(row[:, 0:4, :] - log_total[None])
    columns = columns_of(gain, gain * (row[:, 4:8, :] - delta[None]), 4)
    for h in range(HEADS):
        attn_rows = jnp.zeros((32, HD), F32)
        grad_rows = jnp.zeros((32, HD), F32)
        for s in range(4):
            gain_s = columns[:, s * 8 + h : s * 8 + h + 1]
            tilt_s = columns[:, s * 8 + 4 + h : s * 8 + 5 + h]
            part = rx[h, s].astype(F32)
            attn_rows = attn_rows + gain_s * part[:, 0:HD]
            grad_rows = grad_rows + (tilt_s * part[:, HD : 2 * HD] + gain_s * part[:, 2 * HD :])
        fb[pl.ds(h, 32, stride=8), :] = attn_rows
        fb[pl.ds(HEADS + h, 32, stride=8), :] = grad_rows * SCALE
    sy[...] = fb[...].astype(BF16).reshape(32, 8, HD)

    me = zl * 8 + q

    def row_send(dz, dy, dk):
        kp = lax.rem(k + dk, 2)
        remote(
            sy.at[zs[dz] * 8 + kp * 4 + ys[dy]], ry.at[me], ysend.at[0], yrecv.at[0],
            (ys[dy] * 2 + lax.rem(zh + k, 2), ctx_of(x, zs[dz], kp)),
        ).start()

    for dy in (2, 1, 3, 0):
        for dz in (0, 1, 3, 2):
            for dk in (0, 1):
                if dz or dy or dk:
                    row_send(dz, dy, dk)
        if dy == 1:
            @pl.when(second)
            def _():
                row_send(0, 0, 0)

    @pl.when(first)
    def _():
        ry[pl.ds(me, 1)] = sy[pl.ds(zl * 8 + y, 1)]

    for h in range(HEADS):
        cols = slice(h * HD, (h + 1) * HD)
        factor = jnp.exp(mx[h : h + 1, :] - log_total[h : h + 1])
        center = delta[h : h + 1]
        for rows in chunks[::-1]:
            prob = w16[h, rows, :].astype(F32) * factor
            pb[h, rows, :] = prob.astype(BF16)
            dsb[h, rows, :] = (prob * (dp[h, rows, :] - center)).astype(BF16)
        half = len(chunks) // 2
        for n, rows in enumerate(chunks[half:]):
            xs[h, 0, chunks[n], :] = (dot(dsb[h, rows, :], rows_of(0, h)) * SCALE).astype(BF16)
            xs[h, 1, chunks[n], :] = dot(pb[h, rows, :], rows_of(1, h)).astype(BF16)
        remote(xs.at[h], xr.at[h], gsend.at[0], grecv.at[h], partner).start()
        for rows in chunks[:half]:
            kvo[0, rows, cols] = dot(dsb[h, rows, :], rows_of(0, h)) * SCALE
            kvo[1, rows, cols] = dot(pb[h, rows, :], rows_of(1, h))
    for h in range(HEADS):
        cols = slice(h * HD, (h + 1) * HD)
        await_recv(xr.at[h], grecv.at[h])
        kg_ref[:, cols] = (kvo[0, :, cols] + xr[h, 0].astype(F32)).astype(BF16)
        vg_ref[:, cols] = (kvo[1, :, cols] + xr[h, 1].astype(F32)).astype(BF16)

    @pl.when(first)
    def _():
        await_recv(ry.at[0:31], yrecv.at[0])

    @pl.when(second)
    def _():
        await_recv(ry, yrecv.at[0])

    final = jnp.sum(ry[...].astype(F32).reshape(4, 8, 8, HD), axis=0)
    for qd in range(8):
        for h in range(HEADS):
            cols = slice((qd * HEADS + h) * HD, (qd * HEADS + h + 1) * HD)
            attn_ref[:, cols] = final[qd, h : h + 1, :].astype(BF16)
            dq_ref[:, cols] = final[qd, HEADS + h : HEADS + h + 1, :].astype(BF16)

    for copy in swaps:
        copy.wait_send()
    await_send(sx.at[0:15], xsend.at[0])
    await_send(sf.at[:, 0:3], fsend.at[0])
    await_send(xs, gsend.at[0])

    @pl.when(first)
    def _():
        await_send(gat.at[:, :, 0:3], bsend.at[0])
        await_send(sy.at[0:31], ysend.at[0])

    @pl.when(second)
    def _():
        await_send(sy, ysend.at[0])

    @pl.when(jnp.logical_and(second, edge))
    def _():
        await_send(own, bsend.at[0])


def write_out(attn_in, dq_in, kg_in, vg_in, attn_out, dq_out, kg_out, vg_out, sems):
    pairs = ((kg_in, kg_out), (vg_in, vg_out), (attn_in, attn_out), (dq_in, dq_out))
    copies = [pltpu.make_async_copy(a, b, sems.at[n]) for n, (a, b) in enumerate(pairs)]
    for copy in copies:
        copy.start()
    for copy in copies:
        copy.wait()


def local(query_states, key_states, value_states, level_ids, level_bias, live_counts, out_grad):
    hbm = pl.BlockSpec(memory_space=pltpu.HBM)
    vmem = pl.BlockSpec(memory_space=pltpu.VMEM)
    dma = pltpu.SemaphoreType.DMA
    arrays = (
        query_states, key_states, value_states, level_ids, level_bias, live_counts, out_grad
    )
    shapes = ((1, 3072), (1, 3072), key_states.shape, value_states.shape)
    results = pl.pallas_call(
        kernel,
        name="framepack",
        out_shape=tuple(pltpu.VMEM(shape, BF16) for shape in shapes),
        in_specs=[hbm] * 5 + [pl.BlockSpec(memory_space=pl.ANY), hbm],
        out_specs=(vmem,) * 4,
        scratch_shapes=[
            pltpu.VMEM((2, 32, 3072), BF16),
            pltpu.VMEM((HEADS, 2, 4, 32, HD), BF16),
            pltpu.VMEM((2, BOTH, COLS), BF16),
            pltpu.VMEM((HEADS, 2 * HD, BOTH), BF16),
            pltpu.VMEM((2, HEADS * RUNS + 8, HD), F32),
            pltpu.VMEM((HEADS, BOTH, HD), F32),
            pltpu.VMEM((HD, HD), F32),
            pltpu.VMEM((BOTH, ROWS), F32),
            pltpu.VMEM((HEADS, BOTH, ROWS), BF16),
            pltpu.VMEM((HEADS, BOTH, ROWS), F32),
            pltpu.VMEM((HEADS, BOTH, ROWS), BF16),
            pltpu.VMEM((HEADS, BOTH, ROWS), BF16),
            pltpu.VMEM((8, ROWS), F32),
            pltpu.VMEM((16, 8, HD), F32),
            pltpu.VMEM((HEADS, 4, 32, COLS), BF16),
            pltpu.VMEM((HEADS, 4, 32, COLS), BF16),
            pltpu.VMEM((32 * 8, HD), F32),
            pltpu.VMEM((32, 8, HD), BF16),
            pltpu.VMEM((32, 8, HD), BF16),
            pltpu.VMEM((2, SLOTS, COLS), F32),
            pltpu.VMEM((HEADS, 2, SLOTS, HD), BF16),
            pltpu.VMEM((HEADS, 2, SLOTS, HD), BF16),
            pltpu.SMEM((SLOTS,), jnp.int32),
            pltpu.SMEM((5, 24), F32),
            pltpu.SMEM((1,), jnp.int32),
            dma((7,)),
            dma((3,)), dma((3,)),
            dma((1,)), dma((HEADS,)),
            dma((1,)), dma((1,)),
            pltpu.SemaphoreType.REGULAR,
            dma((1,)), dma((HEADS,)),
            dma((1,)), dma((1,)),
            dma((1,)), dma((HEADS,)),
        ],
        compiler_params=pltpu.CompilerParams(
            collective_id=0, has_side_effects=True, vmem_limit_bytes=40 * 1024 * 1024
        ),
    )(*(a if a is live_counts else pltpu.with_memory_space_constraint(a, pltpu.HBM) for a in arrays))
    return pl.pallas_call(
        write_out,
        name="write_out",
        out_shape=tuple(jax.ShapeDtypeStruct(shape, BF16) for shape in shapes),
        in_specs=[vmem] * 4,
        out_specs=(hbm,) * 4,
        scratch_shapes=[dma((4,))],
    )(*(pltpu.with_memory_space_constraint(a, pltpu.VMEM) for a in results))


def solution(mesh):
    placed = (
        P("query", None),
        P("ctx", "query"),
        P("ctx", "query"),
        P("ctx"),
        P(),
        P("ctx"),
        P("query", None),
    )
    return jax.shard_map(
        local,
        mesh=mesh,
        in_specs=placed,
        out_specs=(
            P(("query", "ctx"), None),
            P(("query", "ctx"), None),
            P("ctx", "query"),
            P("ctx", "query"),
        ),
        check_vma=False,
    )
```

```python
import math

import jax
import jax.numpy as jnp
from jax import lax
from jax.experimental import pallas as pl
from jax.experimental.pallas import tpu as pltpu
from jax.sharding import PartitionSpec as P

MESH = pl.DeviceIdType.MESH
F32 = jnp.float32
BF16 = jnp.bfloat16
HD = 128
HEADS = 3
COLS = HEADS * HD
ROWS = 128
SLOTS = 1024
BOTH = 2 * SLOTS
RUNS = SLOTS // 16
CHUNK = 256
SCALE = 1.0 / math.sqrt(HD)
NT = (((1,), (1,)), ((), ()))
DEAD = -1e30
LOG2E = math.log2(math.e)


def dot_nt(a, b):
    return lax.dot_general(a, b, NT, preferred_element_type=F32)


def dot(a, b):
    return jnp.dot(a, b, preferred_element_type=F32)


def kernel(
    q_hbm, k_hbm, v_hbm, lid_hbm, lb_hbm, lc_hbm, g_hbm,
    attn_ref, dq_ref, kg_ref, vg_ref,
    own, gat, kv, kvt, table, bias, perm, work, w16, dp, pb, dsb, mx,
    sx, sf, rx, fb, sy, ry, kvo, xs, xr, lid, lb, lc,
    ld, dsend, drecv, bsend, brecv, xsend, xrecv, token,
    fsend, frecv, ysend, yrecv, gsend, grecv,
):
    q = lax.axis_index("query")
    c = lax.axis_index("ctx")
    y, zh = q // 2, q % 2
    x, zl, k = c // 8, (c // 2) % 4, c % 2
    first, second = k == 0, k == 1

    def ctx_of(xx, zz, kk):
        return xx * 8 + zz * 2 + kk

    def load(src, dst, n):
        copy = pltpu.make_async_copy(src, dst, ld.at[n])
        copy.start()
        return copy

    loads = [
        load(q_hbm, own.at[0], 0),
        load(g_hbm, own.at[1], 1),
        load(lid_hbm, lid, 2),
        load(lb_hbm, lb, 3),
        load(lc_hbm, lc, 4),
        load(k_hbm, kv.at[0, 0:SLOTS], 5),
        load(v_hbm, kv.at[1, 0:SLOTS], 6),
    ]

    edge = zl % 3 == 0
    near, far = 3 - zl, 2 - zl // 3
    partner = (q, ctx_of(x, zl, 1 - k))
    ys = [lax.rem(y + d, 4) for d in range(4)]
    xs_of = [lax.rem(x + d, 4) for d in range(4)]
    zs = [lax.rem(zl + d, 4) for d in range(4)]
    barrier = pltpu.get_barrier_semaphore()

    def greet(device):
        pl.semaphore_signal(barrier, inc=1, device_id=device, device_id_type=MESH)

    @pl.when(jnp.logical_and(second, edge))
    def _():
        for d in (2, 1, 3, 0):
            greet((ys[d] * 2 + 1 - zh, ctx_of(x, far, 1)))
            greet((ys[d] * 2 + 1 - zh, ctx_of(x, near, 1)))

    @pl.when(jnp.logical_and(second, jnp.logical_not(edge)))
    def _():
        for d in (2, 1, 3, 0):
            greet((ys[d] * 2 + 1 - zh, ctx_of(x, jnp.where(zl < 2, 3, 0), 1)))

    for d in range(1, 4):
        greet((q, ctx_of(x, zs[d], 0)))
        greet((q, ctx_of(x, zs[d], 1)))
        greet((q, ctx_of(xs_of[d], zl, k)))
    greet(partner)

    @pl.when(first)
    def _():
        for d in range(1, 4):
            greet((ys[d] * 2 + zh, c))
        pl.semaphore_wait(barrier, 13)

    @pl.when(second)
    def _():
        pl.semaphore_wait(barrier, 14 + 4 * edge.astype(jnp.int32))

    for d in range(1, 4):
        pl.semaphore_signal(
            token, inc=1, device_id=(q, ctx_of(xs_of[d], zl, k)), device_id_type=MESH
        )

    loads[0].wait()
    loads[1].wait()

    def remote(src, dst, send, recv, device):
        return pltpu.make_async_remote_copy(
            src_ref=src, dst_ref=dst, send_sem=send, recv_sem=recv,
            device_id=device, device_id_type=MESH,
        )

    def block_send(h, yd, half, zz):
        qd = yd * 2 + half
        cols = pl.ds(pl.multiple_of(qd * COLS + h * HD, HD), HD)
        remote(
            own.at[:, :, cols], gat.at[h, :, y], bsend.at[0], brecv.at[h],
            (qd, ctx_of(x, zz, k)),
        ).start()

    @pl.when(first)
    def _():
        for h in range(HEADS):
            for d in (2, 1, 3):
                block_send(h, ys[d], zh, zl)
            cols = pl.ds(pl.multiple_of(q * COLS + h * HD, HD), HD)
            gat[h, :, pl.ds(y, 1)] = own[:, :, cols].reshape(2, 1, 32, HD)

    @pl.when(jnp.logical_and(second, edge))
    def _():
        for h in range(HEADS):
            for d in (2, 1, 3, 0):
                block_send(h, ys[d], 1 - zh, far)
                block_send(h, ys[d], 1 - zh, near)

    loads[2].wait()
    loads[3].wait()
    loads[4].wait()

    def fill(t, carry):
        level = lid[t * 16]
        for h in range(HEADS):
            table[0, pl.ds(h * RUNS + t, 1), :] = jnp.full(
                (1, HD), lb[level, q * HEADS + h] * LOG2E, F32
            )
        return carry

    lax.fori_loop(0, RUNS, fill, 0)
    table[0, HEADS * RUNS :, :] = jnp.full((8, HD), lc[0].astype(F32), F32)
    loads[5].wait()
    loads[6].wait()
    swaps = [
        remote(table.at[0], table.at[1], dsend.at[0], drecv.at[0], partner),
        remote(kv.at[0, 0:SLOTS], kv.at[0, SLOTS:BOTH], dsend.at[1], drecv.at[1], partner),
        remote(kv.at[1, 0:SLOTS], kv.at[1, SLOTS:BOTH], dsend.at[2], drecv.at[2], partner),
    ]
    for copy in swaps:
        copy.start()

    p_id = lax.broadcasted_iota(jnp.int32, (HD, HD), 0)
    i_id = lax.broadcasted_iota(jnp.int32, (HD, HD), 1)
    perm[...] = jnp.where(i_id == ((p_id & 3) << 5) + (p_id >> 2), 1.0, 0.0)
    fb[...] = jnp.zeros_like(fb)
    here = zl * 4 + x
    sx[pl.ds(here, 1)] = jnp.zeros((1, 8, HD), F32)

    def prepare(part):
        def spread(t, carry):
            slot = lax.broadcasted_iota(jnp.int32, (16, HD), 0) + t * 16
            alive = slot.astype(F32) < table[part, HEADS * RUNS : HEADS * RUNS + 1, :]
            at = pl.ds(pl.multiple_of(part * SLOTS + t * 16, 16), 16)
            for h in range(HEADS):
                bias[h, at, :] = jnp.where(alive, table[part, pl.ds(h * RUNS + t, 1), :], DEAD)
            return carry

        lax.fori_loop(0, RUNS, spread, 0, unroll=4)
        for a in range(2):
            for h in range(HEADS):
                for t in range(SLOTS // CHUNK):
                    rows = slice(part * SLOTS + t * CHUNK, part * SLOTS + (t + 1) * CHUNK)
                    kvt[h, (1 - a) * HD : (2 - a) * HD, rows] = kv[a, rows, h * HD : (h + 1) * HD].T

    prepare(0)
    for copy in swaps:
        copy.wait_recv()
    prepare(1)

    chunks = [slice(t * CHUNK, (t + 1) * CHUNK) for t in range(BOTH // CHUNK)]

    def rows_of(a, h):
        return gat[h, a].reshape(ROWS, HD)

    def forward(h):
        cols = slice(h * HD, (h + 1) * HD)
        queries = rows_of(0, h)
        peak = jnp.full((1, HD), DEAD, F32)
        for rows in chunks:
            score = dot_nt(kv[0, rows, cols], queries) * (SCALE * LOG2E) + bias[h, rows, :]
            work[rows, :] = score
            peak = jnp.maximum(peak, jnp.max(score, axis=0, keepdims=True))
        total = jnp.zeros((1, HD), F32)
        for rows in chunks:
            weight = jnp.exp2(work[rows, :] - peak)
            w16[h, rows, :] = weight.astype(BF16)
            total = total + jnp.sum(weight, axis=0, keepdims=True)
        inverse = 1.0 / total
        mixed = dot(kvt[h], w16[h]) * inverse
        grads = rows_of(1, h).T.astype(F32)
        mean = jnp.sum(mixed[0:HD] * grads, axis=0, keepdims=True)
        peak = peak * (1.0 / LOG2E)
        mx[h : h + 1, :] = peak
        sx[pl.ds(here, 1), h : h + 1, :] = (peak + jnp.log(total)).reshape(1, 1, HD)
        sx[pl.ds(here, 1), 4 + h : 5 + h, :] = mean.reshape(1, 1, HD)
        return mixed.astype(BF16), mean, inverse

    def send_shares(h):
        for d in (2, 1, 3):
            remote(
                sf.at[h, xs_of[d]], rx.at[h, x], fsend.at[0], frecv.at[h],
                (q, ctx_of(xs_of[d], zl, k)),
            ).start()

    def shares(h, kept):
        cols = slice(h * HD, (h + 1) * HD)
        mixed, mean, inverse = kept
        turn = perm[...].astype(BF16)
        grads = rows_of(1, h)
        for rows in chunks:
            dprob = dot_nt(kv[1, rows, cols], grads)
            dp[h, rows, :] = dprob
            dsb[h, rows, :] = (w16[h, rows, :].astype(F32) * (dprob - mean)).astype(BF16)
        slope = (dot(kvt[h, HD : 2 * HD, :], dsb[h]) * inverse).astype(BF16)
        turned = jnp.concatenate([mixed, slope], axis=0)
        sf[h] = dot_nt(turn, turned).astype(BF16).reshape(4, 32, COLS)
        send_shares(h)

    def await_recv(ref, sem):
        remote(ref, ref, sem, sem, partner).wait_recv()

    def await_send(ref, sem):
        remote(ref, ref, sem, sem, partner).wait_send()

    kept = []
    for h in range(HEADS):
        @pl.when(first)
        def _():
            await_recv(gat.at[h, :, 0:3], brecv.at[h])

        @pl.when(second)
        def _():
            await_recv(gat.at[h], brecv.at[h])

        kept.append(forward(h))
        if h < 2:
            shares(h, kept[h])
    pl.semaphore_wait(token, 3)
    for dx in (2, 1, 3, 0):
        for dz in (2, 1, 3, 0):
            if dz or dx:
                remote(
                    sx.at[here], sx.at[here], xsend.at[0], xrecv.at[0],
                    (q, ctx_of(xs_of[dx], zs[dz], k)),
                ).start()
    shares(2, kept[2])

    def merge(parts):
        logs, means = parts[:, 0:4, :], parts[:, 4:8, :]
        top = jnp.max(logs, axis=0)
        share = jnp.exp(logs - top[None])
        whole = jnp.sum(share, axis=0)
        return top + jnp.log(whole), jnp.sum(share * means, axis=0) / whole

    own_rows = lax.broadcasted_iota(jnp.int32, (32, HD), 0) + x * 32
    own_lane = ((own_rows & 3) << 5) + (own_rows >> 2)
    pick = jnp.where(lax.broadcasted_iota(jnp.int32, (32, HD), 1) == own_lane, 1.0, 0.0)

    def columns_of(gain, tilt, n):
        both = jnp.concatenate([gain, tilt], axis=-2).reshape(n * 8, HD)
        return lax.dot_general(
            pick, both, NT, preferred_element_type=F32, precision=lax.Precision.HIGHEST
        )

    for h in range(HEADS):
        rx[h, pl.ds(x, 1)] = sf[h, pl.ds(x, 1)]
        await_recv(rx.at[h, 0:3], frecv.at[h])
    await_recv(sx.at[0:15], xrecv.at[0])
    log_total, delta = merge(sx[...])
    row = sx[pl.ds(zl * 4, 4)]
    gain = jnp.exp(row[:, 0:4, :] - log_total[None])
    columns = columns_of(gain, gain * (row[:, 4:8, :] - delta[None]), 4)
    for h in range(HEADS):
        attn_rows = jnp.zeros((32, HD), F32)
        grad_rows = jnp.zeros((32, HD), F32)
        for s in range(4):
            gain_s = columns[:, s * 8 + h : s * 8 + h + 1]
            tilt_s = columns[:, s * 8 + 4 + h : s * 8 + 5 + h]
            part = rx[h, s].astype(F32)
            attn_rows = attn_rows + gain_s * part[:, 0:HD]
            grad_rows = grad_rows + (tilt_s * part[:, HD : 2 * HD] + gain_s * part[:, 2 * HD :])
        fb[pl.ds(h, 32, stride=8), :] = attn_rows
        fb[pl.ds(HEADS + h, 32, stride=8), :] = grad_rows * SCALE
    sy[...] = fb[...].astype(BF16).reshape(32, 8, HD)

    me = zl * 8 + q

    def row_send(dz, dy, dk):
        kp = lax.rem(k + dk, 2)
        remote(
            sy.at[zs[dz] * 8 + kp * 4 + ys[dy]], ry.at[me], ysend.at[0], yrecv.at[0],
            (ys[dy] * 2 + lax.rem(zh + k, 2), ctx_of(x, zs[dz], kp)),
        ).start()

    for dy in (2, 1, 3, 0):
        for dz in (0, 1, 3, 2):
            for dk in (0, 1):
                if dz or dy or dk:
                    row_send(dz, dy, dk)
        if dy == 1:
            @pl.when(second)
            def _():
                row_send(0, 0, 0)

    @pl.when(first)
    def _():
        ry[pl.ds(me, 1)] = sy[pl.ds(zl * 8 + y, 1)]

    for h in range(HEADS):
        cols = slice(h * HD, (h + 1) * HD)
        factor = jnp.exp(mx[h : h + 1, :] - log_total[h : h + 1])
        center = delta[h : h + 1]
        for rows in chunks[::-1]:
            prob = w16[h, rows, :].astype(F32) * factor
            pb[h, rows, :] = prob.astype(BF16)
            dsb[h, rows, :] = (prob * (dp[h, rows, :] - center)).astype(BF16)
        half = len(chunks) // 2
        for n, rows in enumerate(chunks[half:]):
            xs[h, 0, chunks[n], :] = (dot(dsb[h, rows, :], rows_of(0, h)) * SCALE).astype(BF16)
            xs[h, 1, chunks[n], :] = dot(pb[h, rows, :], rows_of(1, h)).astype(BF16)
        remote(xs.at[h], xr.at[h], gsend.at[0], grecv.at[h], partner).start()
        for rows in chunks[:half]:
            kvo[0, rows, cols] = dot(dsb[h, rows, :], rows_of(0, h)) * SCALE
            kvo[1, rows, cols] = dot(pb[h, rows, :], rows_of(1, h))
    for h in range(HEADS):
        cols = slice(h * HD, (h + 1) * HD)
        await_recv(xr.at[h], grecv.at[h])
        kg_ref[:, cols] = (kvo[0, :, cols] + xr[h, 0].astype(F32)).astype(BF16)
        vg_ref[:, cols] = (kvo[1, :, cols] + xr[h, 1].astype(F32)).astype(BF16)

    @pl.when(first)
    def _():
        await_recv(ry.at[0:31], yrecv.at[0])

    @pl.when(second)
    def _():
        await_recv(ry, yrecv.at[0])

    final = jnp.sum(ry[...].astype(F32).reshape(4, 8, 8, HD), axis=0)
    for qd in range(8):
        for h in range(HEADS):
            cols = slice((qd * HEADS + h) * HD, (qd * HEADS + h + 1) * HD)
            attn_ref[:, cols] = final[qd, h : h + 1, :].astype(BF16)
            dq_ref[:, cols] = final[qd, HEADS + h : HEADS + h + 1, :].astype(BF16)

    for copy in swaps:
        copy.wait_send()
    await_send(sx.at[0:15], xsend.at[0])
    await_send(sf.at[:, 0:3], fsend.at[0])
    await_send(xs, gsend.at[0])

    @pl.when(first)
    def _():
        await_send(gat.at[:, :, 0:3], bsend.at[0])
        await_send(sy.at[0:31], ysend.at[0])

    @pl.when(second)
    def _():
        await_send(sy, ysend.at[0])

    @pl.when(jnp.logical_and(second, edge))
    def _():
        await_send(own, bsend.at[0])


def write_out(attn_in, dq_in, kg_in, vg_in, attn_out, dq_out, kg_out, vg_out, sems):
    pairs = ((kg_in, kg_out), (vg_in, vg_out), (attn_in, attn_out), (dq_in, dq_out))
    copies = [pltpu.make_async_copy(a, b, sems.at[n]) for n, (a, b) in enumerate(pairs)]
    for copy in copies:
        copy.start()
    for copy in copies:
        copy.wait()


def local(query_states, key_states, value_states, level_ids, level_bias, live_counts, out_grad):
    hbm = pl.BlockSpec(memory_space=pltpu.HBM)
    vmem = pl.BlockSpec(memory_space=pltpu.VMEM)
    dma = pltpu.SemaphoreType.DMA
    arrays = (
        query_states, key_states, value_states, level_ids, level_bias, live_counts, out_grad
    )
    shapes = ((1, 3072), (1, 3072), key_states.shape, value_states.shape)
    results = pl.pallas_call(
        kernel,
        name="framepack",
        out_shape=tuple(pltpu.VMEM(shape, BF16) for shape in shapes),
        in_specs=[hbm] * 5 + [pl.BlockSpec(memory_space=pl.ANY), hbm],
        out_specs=(vmem,) * 4,
        scratch_shapes=[
            pltpu.VMEM((2, 32, 3072), BF16),
            pltpu.VMEM((HEADS, 2, 4, 32, HD), BF16),
            pltpu.VMEM((2, BOTH, COLS), BF16),
            pltpu.VMEM((HEADS, 2 * HD, BOTH), BF16),
            pltpu.VMEM((2, HEADS * RUNS + 8, HD), F32),
            pltpu.VMEM((HEADS, BOTH, HD), F32),
            pltpu.VMEM((HD, HD), F32),
            pltpu.VMEM((BOTH, ROWS), F32),
            pltpu.VMEM((HEADS, BOTH, ROWS), BF16),
            pltpu.VMEM((HEADS, BOTH, ROWS), F32),
            pltpu.VMEM((HEADS, BOTH, ROWS), BF16),
            pltpu.VMEM((HEADS, BOTH, ROWS), BF16),
            pltpu.VMEM((8, ROWS), F32),
            pltpu.VMEM((16, 8, HD), F32),
            pltpu.VMEM((HEADS, 4, 32, COLS), BF16),
            pltpu.VMEM((HEADS, 4, 32, COLS), BF16),
            pltpu.VMEM((32 * 8, HD), F32),
            pltpu.VMEM((32, 8, HD), BF16),
            pltpu.VMEM((32, 8, HD), BF16),
            pltpu.VMEM((2, SLOTS, COLS), F32),
            pltpu.VMEM((HEADS, 2, SLOTS, HD), BF16),
            pltpu.VMEM((HEADS, 2, SLOTS, HD), BF16),
            pltpu.SMEM((SLOTS,), jnp.int32),
            pltpu.SMEM((5, 24), F32),
            pltpu.SMEM((1,), jnp.int32),
            dma((7,)),
            dma((3,)), dma((3,)),
            dma((1,)), dma((HEADS,)),
            dma((1,)), dma((1,)),
            pltpu.SemaphoreType.REGULAR,
            dma((1,)), dma((HEADS,)),
            dma((1,)), dma((1,)),
            dma((1,)), dma((HEADS,)),
        ],
        compiler_params=pltpu.CompilerParams(
            collective_id=0, has_side_effects=True, vmem_limit_bytes=40 * 1024 * 1024
        ),
    )(*(a if a is live_counts else pltpu.with_memory_space_constraint(a, pltpu.HBM) for a in arrays))
    return pl.pallas_call(
        write_out,
        name="write_out",
        out_shape=tuple(jax.ShapeDtypeStruct(shape, BF16) for shape in shapes),
        in_specs=[vmem] * 4,
        out_specs=(hbm,) * 4,
        scratch_shapes=[dma((4,))],
    )(*(pltpu.with_memory_space_constraint(a, pltpu.VMEM) for a in results))


def solution(mesh):
    placed = (
        P("query", None),
        P("ctx", "query"),
        P("ctx", "query"),
        P("ctx"),
        P(),
        P("ctx"),
        P("query", None),
    )
    return jax.shard_map(
        local,
        mesh=mesh,
        in_specs=placed,
        out_specs=(
            P(("query", "ctx"), None),
            P(("query", "ctx"), None),
            P("ctx", "query"),
            P("ctx", "query"),
        ),
        check_vma=False,
    )
```
